32 devices in a mesh: gx: 16 (over z, y, x), gy: 2 (over core).
Axes of the slice: x: 2, y: 2, z: 4, core: 2. Of those that a mesh axis runs over, the one named last changes fastest.
Arguments:
- operator: float32 [243, 32768], P(None, ('gx', 'gy')), may hold values from -0.6 to 10.6
- basis_u: float32 [144, 32768], P(None, ('gx', 'gy')), may hold values from -6 to 6
- basis_c: float32 [144, 32768], P(None, ('gx', 'gy')), may hold values from -6 to 6
- right_side: float32 [3, 32768], P(None, ('gx', 'gy')), may hold values from -16 to 16
- new_rows: int32 [32768], P(('gx', 'gy')), may hold values from 0 to 32767, as said below
Outputs:
- solution: float32 [3, 32768], P(None, ('gx', 'gy'))
- residual: float32 [3, 32768], P(None, ('gx', 'gy'))
The draws below stay inside these ranges and needn't reach their ends.
Inputs may be any that keep to these rules, and one draw needn't show every extreme that they name: `new_rows`: each block row gets one new index (a permutation). Each device sends 0 to 64 of its old rows to each device, and each device both sends exactly 64 rows to some peer and receives exactly 64 rows from some peer.
All inputs are finite; a program needn't handle non-finite values.
Results may differ from the reference program's by a relative error of at most 0.0003.
Values sent between devices are 32-bit elements; how exact they have to be, the bound alone decides.
A program may use at most 64 MiB of HBM per device.

```python
import jax
import jax.numpy as jnp
from jax import lax

CX = 1
CY = 8
CZ = 128
K = 48
ROWS_DEV = 1024
PEERS = 32
ROWS = 32768
N_GX = 16
N_GY = 2


def c_values(key):
    values = jnp.clip(jax.random.normal(jax.random.fold_in(key, 11), (3 * K, ROWS), jnp.float32), -6.0, 6.0)
    return values


def draw_basis_c(key, part):
    return c_values(key)


def draw_right_side(key, part):
    values = c_values(key).reshape(3, K, ROWS)
    weights = jax.random.normal(jax.random.fold_in(key, 13), (K,), jnp.float32) / jnp.sqrt(1.0 * K)
    along = jnp.einsum('amp,m->ap', values, weights)
    owner = (draw_new_rows(key, part) // ROWS_DEV).astype(jnp.float32)
    place = owner / (1.0 * (PEERS - 1))
    noise = jax.random.normal(jax.random.fold_in(key, 12), (3, ROWS), jnp.float32)
    rising = 1.0 + 4.0 * place
    return jnp.clip(noise * rising[None, :] + along, -16.0, 16.0)


def draw_operator(key, part):
    off = jnp.clip(0.1 * jax.random.normal(jax.random.fold_in(key, 21), (27, 3, 3, ROWS), jnp.float32), -0.6, 0.6)
    diag = 6.0 + 4.0 * jax.random.uniform(jax.random.fold_in(key, 22), (3, ROWS), jnp.float32)
    eye = jnp.eye(3, dtype=jnp.float32)
    off = off.at[13].add(eye[:, :, None] * diag[:, None, :])
    return off.reshape(243, ROWS)


def draw_new_rows(key, part):
    peers = PEERS
    rows = ROWS_DEV
    base = rows // peers
    half = jax.random.randint(jax.random.fold_in(key, 31), (peers // 2,), -base, base + 1)
    half = half.at[0].set(base)
    sizes = base + jnp.concatenate([half, -half])
    sigma = jax.random.permutation(jax.random.fold_in(key, 32), peers)
    tau = jax.random.permutation(jax.random.fold_in(key, 33), peers)
    counts = sizes[(sigma[:, None] + tau[None, :]) % peers]
    offsets = jnp.cumsum(counts, 0) - counts
    ends = jnp.cumsum(counts, 1)
    starts = ends - counts
    keys = jax.random.split(jax.random.fold_in(key, 34), peers)
    orders = jax.vmap(lambda k: jax.random.permutation(k, rows))(keys)
    places = jnp.arange(rows, dtype=jnp.int32)

    def one_source(order, end_row, start_row, offset_row):
        target = jnp.searchsorted(end_row, places, side='right').astype(jnp.int32)
        newer = target * rows + offset_row[target] + places - start_row[target]
        return jnp.zeros((rows,), jnp.int32).at[order].set(newer.astype(jnp.int32))
    table = jax.vmap(one_source)(orders, ends, starts, offsets)
    return table.reshape(peers * rows).astype(jnp.int32)


def level_of(key, extent, shards, smallest, high):
    loudness = 1.0
    for dim, blocks in shards:
        draws = jax.random.uniform(jax.random.fold_in(jax.random.fold_in(key, 6), dim), (blocks,), jnp.float32, smallest / len(shards), high / len(shards))
        loudness = loudness * jnp.repeat(jnp.exp(draws), extent[dim] // blocks).reshape((-1,) + (1,) * (len(extent) - 1 - dim))
    return loudness


def gaussian(key, shape, scale, reach, cuts=(), kind=jnp.bfloat16):
    result = jax.random.normal(key, shape, jnp.float32) * scale
    if len(cuts) > 0:
        result = level_of(key, shape, cuts, -0.22, 0.18) * result
    return jnp.clip(result, min=-reach, max=reach).astype(kind)


def setup_inputs(seed: int = 0) -> dict:
    key_of = jax.random.split(jax.random.key(seed), 6)
    return {
        "operator": draw_operator(jax.random.fold_in(key_of[5], 71), 0),
        "basis_u": gaussian(key_of[1], (3 * K, ROWS), 1.0, 6.0, ((1, 32),), jnp.float32),
        "basis_c": draw_basis_c(jax.random.fold_in(key_of[5], 71), 0),
        "right_side": draw_right_side(jax.random.fold_in(key_of[5], 71), 0),
        "new_rows": draw_new_rows(jax.random.fold_in(key_of[5], 71), 0),
    }


def to_grid(values):
    width = values.shape[0]
    shaped = values.reshape(width, N_GX, N_GY, CX, CY, CZ).transpose(0, 1, 3, 2, 4, 5)
    return shaped.reshape(width, N_GX * CX, N_GY * CY, CZ)

def to_rows(grid):
    width = grid.shape[0]
    shaped = grid.reshape(width, N_GX, CX, N_GY, CY, CZ).transpose(0, 1, 3, 2, 4, 5)
    return shaped.reshape(width, ROWS)

def stencil(coef, padded):
    size_x = padded.shape[1] - 2
    size_y = padded.shape[2] - 2
    size_z = padded.shape[3] - 2
    total = jnp.zeros((3, size_x, size_y, size_z), jnp.float32)
    for k in range(27):
        dx, dy, dz = (k // 9, k // 3 % 3, k % 3)
        moved = padded[:, dx:dx + size_x, dy:dy + size_y, dz:dz + size_z]
        total = total + lax.optimization_barrier(jnp.sum(coef[k] * moved[None], axis=1))
    return total

def apply_op(coef, vector):
    padded = jnp.pad(to_grid(vector), ((0, 0), (1, 1), (1, 1), (1, 1)))
    return to_rows(stencil(coef, padded))

def project(basis, vector):
    return jnp.einsum('amp,ap->m', basis, vector, precision=lax.Precision.HIGHEST)

def combine(basis, coeffs):
    return jnp.einsum('amp,m->ap', basis, coeffs, precision=lax.Precision.HIGHEST)

def reference(operator, basis_u, basis_c, right_side, new_rows):
    payload = jnp.concatenate([operator, basis_u, basis_c, right_side], 0)
    moved = jnp.zeros_like(payload).at[:, new_rows].set(payload)
    coef = to_grid(moved[:243]).reshape(27, 3, 3, N_GX * CX, N_GY * CY, CZ)
    u = moved[243:243 + 3 * K].reshape(3, K, ROWS)
    c = moved[243 + 3 * K:243 + 6 * K].reshape(3, K, ROWS)
    b = moved[243 + 6 * K:]
    gram = jnp.einsum('amp,anp->mn', c, c, precision=lax.Precision.HIGHEST)
    lower = jnp.linalg.cholesky(gram)
    lower_inv = jax.scipy.linalg.solve_triangular(lower, jnp.eye(K, dtype=jnp.float32), lower=True)
    cq = jnp.einsum('mn,anp->amp', lower_inv, c, precision=lax.Precision.HIGHEST)
    uq = jnp.einsum('mn,anp->amp', lower_inv, u, precision=lax.Precision.HIGHEST)
    start = project(cq, b)
    first_x = combine(uq, start)
    first_r = b - combine(cq, start)
    beta = jnp.sqrt(jnp.sum(first_r * first_r))
    vec_one = first_r / beta
    image = apply_op(coef, vec_one)
    proj_one = project(cq, image)
    h11 = jnp.sum(vec_one * image)
    rest = image - combine(cq, proj_one) - h11 * vec_one
    h21 = jnp.sqrt(jnp.sum(rest * rest))
    vec_two = rest / h21
    image = apply_op(coef, vec_two)
    proj_two = project(cq, image)
    h12 = jnp.sum(vec_one * image)
    h22 = jnp.sum(vec_two * image)
    rest = image - combine(cq, proj_two) - h12 * vec_one - h22 * vec_two
    h32 = jnp.sqrt(jnp.sum(rest * rest))
    m11 = h11 * h11 + h21 * h21
    m12 = h11 * h12 + h21 * h22
    m22 = h12 * h12 + h22 * h22 + h32 * h32
    g_one = beta * h11
    g_two = beta * h12
    determ = m11 * m22 - m12 * m12
    y_one = (m22 * g_one - m12 * g_two) / determ
    y_two = (m11 * g_two - m12 * g_one) / determ
    solution = first_x + y_one * vec_one + y_two * vec_two - combine(uq, y_one * proj_one + y_two * proj_two)
    residual = b - apply_op(coef, solution)
    return (solution, residual)
```

```python
import functools

import jax
import jax.numpy as jnp
from jax import lax
from jax.experimental import pallas as pl
from jax.experimental.pallas import tpu as pltpu
from jax.sharding import PartitionSpec as P

LN = 128
F32 = jnp.float32
BF16 = jnp.bfloat16
I32 = jnp.int32
HIGH = lax.Precision.HIGHEST
NT = (((1,), (1,)), ((), ()))


class Plan:
    def __init__(self, nx, ny, rows, op_rows, basis_rows):
        self.nx, self.ny, self.rows = nx, ny, rows
        self.peers = nx * ny
        self.k = basis_rows // 3
        self.op_rows, self.basis_rows = op_rows, basis_rows
        self.lines = rows // LN
        self.q = nx * self.lines
        self.qh = self.q // 2
        self.cols = self.peers * self.lines
        self.blocks = self.cols // 256
        self.height = ny * self.lines


def kernel(
    pn, op_ref, u_ref, c_ref, b_ref, nr_ref, sol_ref, res_ref,
    opd, bd, nrb, iacc, itab, kidx, qidx, tab, wd, gpk, grcv, mred, rsnd, rrcv, vsnd, vb,
    n_s, n_r, g_s, g_r, r_s, r_r, v_s, v_r,
):
    gx, gy = lax.axis_index("gx"), lax.axis_index("gy")
    me = gx * pn.ny + gy
    peers, k, lines = pn.peers, pn.k, pn.lines

    def dev(p):
        return {"gx": lax.div(p, pn.ny), "gy": lax.rem(p, pn.ny)}

    def remote(src, dst, ssem, rsem, p):
        return pltpu.make_async_remote_copy(
            src_ref=src, dst_ref=dst, send_sem=ssem, recv_sem=rsem,
            device_id=dev(p), device_id_type=pl.DeviceIdType.MESH,
        )

    def others(body):
        def step(d, _):
            body(lax.rem(me + d, peers))
            return 0
        lax.fori_loop(1, peers, step, 0)

    barrier = pltpu.get_barrier_semaphore()
    others(lambda p: pl.semaphore_signal(
        barrier, inc=1, device_id=dev(p), device_id_type=pl.DeviceIdType.MESH))

    lane = lax.broadcasted_iota(I32, (8, LN), 1)
    sub = lax.broadcasted_iota(I32, (8, LN), 0)
    iota_row = lax.broadcasted_iota(I32, (256, LN), 0).astype(F32).astype(BF16)
    one, zero = jnp.ones((), BF16), jnp.zeros((), BF16)

    def lsum(x):
        return jnp.sum(x, axis=1, keepdims=True)

    def ssum(x):
        return jnp.sum(x, axis=0, keepdims=True)

    def fold(v):
        for h in (4, 2, 1):
            low = (sub & h) == 0
            n = len(v) // 2
            nxt = []
            for i in range(n):
                keep = jnp.where(low, v[i], v[i + n])
                give = jnp.where(low, v[i + n], v[i])
                if h == 4:
                    moved = pltpu.roll(give, 4, 0)
                else:
                    moved = jnp.where(low, pltpu.roll(give, 8 - h, 0), pltpu.roll(give, h, 0))
                nxt.append(keep + moved)
            v = nxt
        return v[0]

    def pick(parts, bits):
        for bit in bits:
            parts = [jnp.where(bit, parts[2 * j + 1], parts[2 * j]) for j in range(len(parts) // 2)]
        return parts[0]

    def onehot(row):
        return jnp.where(iota_row == row, one, zero)

    nrb[me] = nr_ref[...]

    ext = []
    for a in range(3):
        rows_b = jnp.broadcast_to(b_ref[a : a + 1, :], (8, pn.rows))
        ext.append(jnp.concatenate([c_ref[a * k : (a + 1) * k, :], rows_b], axis=0))
    gram = None
    for a in range(3):
        g = lax.dot_general(ext[a], ext[a], NT, precision=HIGH, preferred_element_type=F32)
        gram = g if gram is None else gram + g
    gram = jnp.concatenate([gram, jnp.zeros((k + 8, LN - k - 8), F32)], axis=1)
    lane16 = lax.broadcasted_iota(I32, (16, LN), 1)
    packet = jnp.zeros((16, LN), F32)
    third = k // 3
    groups = [gram[third * i : third * (i + 1)] for i in range(3)]
    tail = jnp.concatenate([gram[k : k + 8], gram[k : k + 8]], axis=0)
    starts = (0, third, 3 * third, 6 * third)
    for i in range(3):
        moved = pltpu.roll(groups[i], starts[i], 1) if starts[i] else groups[i]
        inside = jnp.logical_and(lane16 >= starts[i], lane16 < starts[i + 1])
        packet = jnp.where(inside, moved, packet)
        packet = jnp.where(lane16 == starts[3] + i, pltpu.roll(groups[i], starts[3] + i - k, 1), packet)
    packet = jnp.where(lane16 == starts[3] + 3, pltpu.roll(tail, starts[3] + 3 - k, 1), packet)
    gpk[...] = packet
    grcv[me] = packet

    pl.semaphore_wait(barrier, peers - 1)
    others(lambda p: remote(nr_ref, nrb.at[me], n_s.at[p], n_r.at[me], p).start())
    others(lambda p: remote(gpk, grcv.at[me], g_s.at[p], g_r.at[me], p).start())

    for t in range(lines):
        at = slice(t * LN, (t + 1) * LN)
        opd[pl.ds(t, pn.op_rows, stride=lines), :] = op_ref[:, at]
        bd[pl.ds(t, 3, stride=lines), :] = b_ref[:, at]
    load = [bd[a * lines : (a + 1) * lines, :] for a in range(3)]

    others(lambda p: remote(nr_ref, nrb.at[p], n_s.at[p], n_r.at[p], p).wait_recv())
    for cb in range(pn.blocks):
        iacc[cb] = jnp.zeros((256, 256), F32)
    lane_row = lax.broadcasted_iota(I32, (1, LN), 1)

    def invert(d, _):
        zs = []
        core = lax.rem(d, pn.ny)
        first = (core * LN + lane_row).astype(F32).astype(BF16)
        for s in range(lines):
            row = nrb[d, s : s + 1, :]
            zrow = lax.bitwise_and(row, LN - 1).astype(F32).astype(BF16)
            hit = iota_row[0:LN] == zrow
            line = lax.div(d, pn.ny) * lines + s - pn.qh
            second = jnp.full((1, LN), 0, I32) + line
            second = second.astype(F32).astype(BF16)
            zs.append(jnp.concatenate([jnp.where(hit, first, zero), jnp.where(hit, second, zero)], axis=0))
        z = jnp.concatenate(zs, axis=1)
        for cb in range(pn.blocks):
            cs = []
            for s in range(lines):
                crow = lax.shift_right_logical(nrb[d, s : s + 1, :], 7) - cb * 256
                crow = jnp.clip(crow, -1, 256).astype(F32).astype(BF16)
                cs.append(onehot(crow))
            c = jnp.concatenate(cs, axis=1)
            iacc[cb] += lax.dot_general(z, c, NT, preferred_element_type=F32)
        return 0

    lax.fori_loop(0, peers, invert, 0)
    for cb in range(pn.blocks):
        itab[cb] = iacc[cb].astype(BF16)

    others(lambda p: remote(gpk, grcv.at[p], g_s.at[p], g_r.at[p], p).wait_recv())
    total = grcv[0]
    for d in range(1, peers):
        total = total + grcv[d]
    ke = k + 8
    lanes_e = lax.broadcasted_iota(I32, (ke, LN), 1)
    rows_e = lax.broadcasted_iota(I32, (ke, LN), 0)
    low = []
    for i in range(3):
        block = pltpu.roll(total, LN - starts[i], 1) if starts[i] else total
        block = jnp.where(lane16 < third * (i + 1), block, 0.0)
        load_col = pltpu.roll(total, LN - (starts[3] + i) + k, 1)
        low.append(jnp.where(lane16 == k, load_col, block))
    square = pltpu.roll(total, LN - (starts[3] + 3) + k, 1)
    low.append(jnp.where(lane16 == k, square, 0.0)[0:8])
    low.append(jnp.zeros((LN - ke, LN), F32))
    low = jnp.concatenate(low, axis=0)
    high = jnp.transpose(low)
    low, high = low[0:ke], high[0:ke]
    diag = lax.div(rows_e, third) == lax.div(lanes_e, third)
    lower = jnp.logical_or(diag, lanes_e <= rows_e)
    mat = jnp.where(jnp.logical_or(lower, lanes_e == k), low, high)
    mat = jnp.where(jnp.logical_and(rows_e == k, lanes_e < k), high, mat)
    for i in range(k):
        row = mat[i : i + 1, :]
        col = jnp.broadcast_to(mat[:, i : i + 1], (ke, LN))
        at = lanes_e == i
        scaled = jnp.where(lane_row == i, 1.0, row) / col[i : i + 1]
        inner = jnp.where(at, 0.0, mat) - col * scaled
        mat = jnp.where(rows_e == i, scaled, inner)
    ginv = jnp.where(lanes_e < k, mat, 0.0)[0:k]
    z0 = jnp.broadcast_to(mat[0:k, k : k + 1], (k, LN))
    beta = jnp.sqrt(jnp.broadcast_to(mat[k : k + 1, k : k + 1], (1, LN)))

    def combine(ref, z):
        out = []
        for a in range(3):
            sums = []
            for t in range(lines):
                s = None
                for g in range(k // 8):
                    term = ref[a * k + 8 * g : a * k + 8 * g + 8, t * LN : (t + 1) * LN] * z[8 * g : 8 * g + 8]
                    s = term if s is None else s + term
                sums.append(s)
            out.append(fold(sums))
        return out

    half_n = pn.nx // 2
    side = lax.div(gx, half_n)

    def spread(phase, v):
        for a in range(3):
            vsnd[phase, a] = v[a]
            vb[phase, gy, a, pl.ds(pl.multiple_of(gx * lines, 8), 8), :] = v[a]
        mine = pl.ds(pl.multiple_of(gx * lines, 8), 8)
        others(lambda p: remote(
            vsnd.at[phase], vb.at[phase, gy, :, mine, :], v_s.at[phase, p], v_r.at[phase, me], p).start())

    def arrive(phase, half):
        def step(i, _):
            p = half * half_n * pn.ny + i
            at = pl.ds(pl.multiple_of(lax.div(p, pn.ny) * lines, 8), 8)

            @pl.when(p != me)
            def _():
                remote(vsnd.at[phase], vb.at[phase, lax.rem(p, pn.ny), :, at, :],
                       v_s.at[phase, p], v_r.at[phase, p], p).wait_recv()
            return 0
        lax.fori_loop(0, half_n * pn.ny, step, 0)
        begin = pl.ds(pl.multiple_of(half * pn.qh, 8), pn.qh)
        for b in range(3):
            for core in range(pn.ny):
                x = vb[phase, core, b, begin, :]
                hi = x.astype(BF16)
                lanes_c = slice(core * LN, (core + 1) * LN)
                tab[b * pn.qh : (b + 1) * pn.qh, lanes_c] = hi
                tab[(3 + b) * pn.qh : (4 + b) * pn.qh, lanes_c] = (x - hi.astype(F32)).astype(BF16)

    levels = pn.qh.bit_length() - 4
    rest = ~((pn.qh - 1) & ~7)

    def gather(kk, half):
        vals = [[None] * lines for _ in range(3)]
        for c in range(lines // 2):
            w = jnp.concatenate(
                [onehot(kidx[kk, 2 * c + t : 2 * c + t + 1, :].astype(BF16)) for t in range(2)], axis=1)
            r = jnp.dot(tab[...], w, preferred_element_type=F32)
            for t in range(2):
                q = jnp.broadcast_to(qidx[kk, 2 * c + t : 2 * c + t + 1, :], (8, LN)) - half * pn.qh
                bits = [lax.bitwise_and(q, 8 << i) != 0 for i in range(levels)]
                here = lax.bitwise_and(q, rest) == sub
                lanes_t = slice(t * LN, (t + 1) * LN)
                for b in range(3):
                    parts = []
                    for i in range(pn.qh // 8):
                        at = b * pn.qh + i * 8
                        lo = 3 * pn.qh + at
                        parts.append(r[at : at + 8, lanes_t] + r[lo : lo + 8, lanes_t])
                    vals[b][2 * c + t] = jnp.where(here, pick(parts, bits), 0.0)
        return [fold(vals[b]) for b in range(3)]

    def coef(i):
        return opd[pl.ds(pl.multiple_of(i * lines, 8), 8), :]

    def apply_half(half):
        def step(kk, out):
            g = gather(kk, half)
            return tuple(
                out[a] + coef(kk * 9 + a * 3) * g[0] + coef(kk * 9 + a * 3 + 1) * g[1] + coef(kk * 9 + a * 3 + 2) * g[2]
                for a in range(3))
        return lax.fori_loop(0, pn.op_rows // 9, step, (jnp.zeros((8, LN), F32),) * 3)

    def apply_op(phase, extra=False):
        def step(i, carry):
            half = lax.rem(side + i, 2)
            arrive(phase, half)
            part = apply_half(half)
            if extra:
                part = part + tuple(gather(pn.op_rows // 9, half))
            return tuple(x + y for x, y in zip(carry, part))
        return lax.fori_loop(0, 2, step, (jnp.zeros((8, LN), F32),) * (6 if extra else 3))

    def dot3(p, q):
        return ssum(p[0] * q[0] + p[1] * q[1] + p[2] * q[2])

    def sums_of(phase, w, vectors):
        for a in range(3):
            wd[a] = w[a]
        bc = [[jnp.broadcast_to(wd[a, t : t + 1, :], (8, LN)) for t in range(lines)] for a in range(3)]
        for g in range(k // 8):
            s = None
            for a in range(3):
                for t in range(lines):
                    term = c_ref[a * k + 8 * g : a * k + 8 * g + 8, t * LN : (t + 1) * LN] * bc[a][t]
                    s = term if s is None else s + term
            mred[8 * g : 8 * g + 8, :] = s
        tail_rows = jnp.zeros((8, LN), F32)
        for i, vector in enumerate(vectors + [w]):
            tail_rows = jnp.where(sub == i, dot3(vector, w), tail_rows)
        mred[k : k + 8, :] = tail_rows
        mred[k + 8 :, :] = jnp.zeros((LN - k - 8, LN), F32)
        mine_row = lax.dot_general(jnp.ones((8, LN), F32), mred[...], NT, precision=HIGH, preferred_element_type=F32)[0:1]
        rsnd[phase] = mine_row
        rrcv[phase, me] = mine_row
        others(lambda p: remote(rsnd.at[phase], rrcv.at[phase, me], r_s.at[phase, p], r_r.at[phase, me], p).start())
        others(lambda p: remote(rsnd.at[phase], rrcv.at[phase, p], r_s.at[phase, p], r_r.at[phase, p], p).wait_recv())
        prow = jnp.sum(rrcv[phase], axis=0)
        pcol = lsum(jnp.where(lanes_e == rows_e, prow, 0.0))
        z = lsum(ginv * prow)
        pz = ssum(pcol[0:k] * z)
        pcol = jnp.broadcast_to(pcol, (ke, LN))
        return jnp.broadcast_to(z, (k, LN)), jnp.broadcast_to(pz, (1, LN)), [pcol[k + i : k + i + 1] for i in range(3)]

    part = combine(c_ref, z0)
    v1 = [(load[a] - part[a]) / beta for a in range(3)]
    spread(0, v1)

    nr = nr_ref[...]
    x_at = lax.div(nr, pn.height * LN)
    y_at = lax.bitwise_and(lax.shift_right_logical(nr, 7), pn.height - 1)
    z_at = lax.bitwise_and(nr, LN - 1)
    zl = LN.bit_length() - 4

    def look(crow_of, zrow_of, shifts):
        vals = [[[None] * lines for _ in range(2)] for _ in shifts]
        for c in range(lines // 2):
            r = None
            for cb in range(pn.blocks):
                w = jnp.concatenate(
                    [onehot(jnp.clip(crow_of(2 * c + t) - cb * 256, -1, 256).astype(F32).astype(BF16)) for t in range(2)],
                    axis=1)
                d = jnp.dot(itab[cb], w, preferred_element_type=F32)
                r = d if r is None else r + d
            for t in range(2):
                for i, dz in enumerate(shifts):
                    zq = jnp.broadcast_to(zrow_of(2 * c + t), (8, LN)) + dz
                    bits = [lax.bitwise_and(zq, 8 << j) != 0 for j in range(zl)]
                    here = lax.bitwise_and(zq, 7) == sub
                    for p in range(2):
                        parts = [r[p * LN + 8 * j : p * LN + 8 * j + 8, t * LN : (t + 1) * LN] for j in range(LN // 8)]
                        vals[i][p][2 * c + t] = jnp.where(here, pick(parts, bits), 0.0)
        return [[fold(vals[i][p]) for p in range(2)] for i in range(len(shifts))]

    def neighbours(j, _):
        dx = lax.div(j, 3) - 1
        dy = lax.rem(j, 3) - 1
        found = look(
            lambda t: lax.shift_right_logical(nr_ref[t : t + 1, :], 7) + (dx * pn.height + dy),
            lambda t: lax.bitwise_and(nr_ref[t : t + 1, :], LN - 1),
            (-1, 0, 1))
        xs, ys = x_at + dx, y_at + dy
        inside = jnp.logical_and(
            jnp.logical_and(xs >= 0, xs < pn.nx), jnp.logical_and(ys >= 0, ys < pn.height))
        for i, dz in enumerate((-1, 0, 1)):
            zs = z_at + dz
            good = jnp.logical_and(inside, jnp.logical_and(zs >= 0, zs < LN))
            kidx[j * 3 + i] = found[i][0]
            qidx[j * 3 + i] = jnp.where(good, found[i][1].astype(I32) + pn.qh, -1)
        return 0

    lax.fori_loop(0, 9, neighbours, 0)
    own = look(
        lambda t: jnp.zeros((1, LN), I32) + (me * lines + t), lambda t: lane_row, (0,))
    kidx[pn.op_rows // 9] = own[0][0]
    qidx[pn.op_rows // 9] = own[0][1].astype(I32) + pn.qh

    w1 = apply_op(0)
    z1, pz, (h11, ww, _) = sums_of(0, w1, [v1])
    h21 = jnp.sqrt(ww - pz - h11 * h11)
    part = combine(c_ref, z1)
    v2 = [(w1[a] - part[a] - h11 * v1[a]) / h21 for a in range(3)]
    spread(1, v2)
    w2 = apply_op(1)
    z2, pz, (h12, h22, ww) = sums_of(1, w2, [v1, v2])
    h32 = jnp.sqrt(ww - pz - h12 * h12 - h22 * h22)
    m11 = h11 * h11 + h21 * h21
    m12 = h11 * h12 + h21 * h22
    m22 = h12 * h12 + h22 * h22 + h32 * h32
    g_one, g_two = beta * h11, beta * h12
    determ = m11 * m22 - m12 * m12
    y_one = (m22 * g_one - m12 * g_two) / determ
    y_two = (m11 * g_two - m12 * g_one) / determ
    ut = combine(u_ref, z0 - y_one * z1 - y_two * z2)
    spread(2, [ut[a] + y_one * v1[a] + y_two * v2[a] for a in range(3)])
    out = apply_op(2, extra=True)
    spread(3, [load[a] - out[a] for a in range(3)])
    for a in range(3):
        sol_ref[a] = out[3 + a]

    def last(i, carry):
        half = lax.rem(side + i, 2)
        arrive(3, half)
        return tuple(x + y for x, y in zip(carry, gather(pn.op_rows // 9, half)))

    out = lax.fori_loop(0, 2, last, (jnp.zeros((8, LN), F32),) * 3)
    for a in range(3):
        res_ref[a] = out[a]

    others(lambda p: remote(nr_ref, nrb.at[me], n_s.at[p], n_r.at[me], p).wait_send())
    others(lambda p: remote(gpk, grcv.at[me], g_s.at[p], g_r.at[me], p).wait_send())
    mine = pl.ds(pl.multiple_of(gx * lines, 8), 8)
    for phase in range(2):
        others(lambda p: remote(rsnd.at[phase], rrcv.at[phase, me], r_s.at[phase, p], r_r.at[phase, me], p).wait_send())
    for phase in range(4):
        others(lambda p: remote(
            vsnd.at[phase], vb.at[phase, gy, :, mine, :], v_s.at[phase, p], v_r.at[phase, me], p).wait_send())


def body(nx, ny, operator, basis_u, basis_c, right_side, new_rows):
    rows = operator.shape[1]
    pn = Plan(nx, ny, rows, operator.shape[0], basis_u.shape[0])
    n, lines = pn.peers, pn.lines
    vmem, dma = pltpu.VMEM, pltpu.SemaphoreType.DMA
    out = jax.ShapeDtypeStruct((3, lines, LN), F32)
    whole = pl.BlockSpec(memory_space=pltpu.VMEM)
    points = pn.op_rows // 9 + 1
    sol, res = pl.pallas_call(
        functools.partial(kernel, pn),
        out_shape=(out, out),
        in_specs=[whole] * 5,
        out_specs=(whole, whole),
        scratch_shapes=[
            vmem((pn.op_rows * lines, LN), F32),
            vmem((3 * lines, LN), F32),
            vmem((n, lines, LN), I32),
            vmem((pn.blocks, 256, 256), F32),
            vmem((pn.blocks, 256, 256), BF16),
            vmem((points, lines, LN), F32),
            vmem((points, lines, LN), I32),
            vmem((6 * pn.qh, 256), BF16),
            vmem((3, lines, LN), F32),
            vmem((16, LN), F32),
            vmem((n, 16, LN), F32),
            vmem((LN, LN), F32),
            vmem((2, 1, LN), F32),
            vmem((2, n, 1, LN), F32),
            vmem((4, 3, lines, LN), F32),
            vmem((4, ny, 3, pn.q, LN), F32),
            dma((n,)), dma((n,)),
            dma((n,)), dma((n,)),
            dma((2, n)), dma((2, n)),
            dma((4, n)), dma((4, n)),
        ],
        compiler_params=pltpu.CompilerParams(
            collective_id=0, has_side_effects=True, vmem_limit_bytes=60 << 20
        ),
        name="solve",
    )(operator, basis_u, basis_c, right_side, new_rows.reshape(lines, LN))
    return sol.reshape(3, rows), res.reshape(3, rows)


def solution(mesh):
    split = P(None, ("gx", "gy"))
    return jax.shard_map(
        functools.partial(body, mesh.shape["gx"], mesh.shape["gy"]),
        mesh=mesh,
        in_specs=(split, split, split, split, P(("gx", "gy"))),
        out_specs=(split, split),
        check_vma=False,
    )
```

```python
import functools

import jax
import jax.numpy as jnp
from jax import lax
from jax.experimental import pallas as pl
from jax.experimental.pallas import tpu as pltpu
from jax.sharding import PartitionSpec as P

LN = 128
F32 = jnp.float32
BF16 = jnp.bfloat16
I32 = jnp.int32
F8 = jnp.float8_e4m3fn
HIGH = lax.Precision.HIGHEST
NT = (((1,), (1,)), ((), ()))


class Plan:
    def __init__(self, nx, ny, rows, op_rows, basis_rows):
        self.nx, self.ny, self.rows = nx, ny, rows
        self.peers = nx * ny
        self.k = basis_rows // 3
        self.op_rows, self.basis_rows = op_rows, basis_rows
        self.lines = rows // LN
        self.q = nx * self.lines
        self.qh = self.q // 2
        self.cols = self.peers * self.lines
        self.blocks = self.cols // 256
        self.height = ny * self.lines


def kernel(
    pn, op_ref, u_ref, c_ref, b_ref, nr_ref, sol_ref, res_ref,
    opd, bd, nrb, iacc, itab, kidx, qidx, tab, sinv, wd, gpk, grcv, mred, rsnd, rrcv, vsnd, vb,
    n_s, n_r, g_s, g_r, r_s, r_r, v_s, v_r,
):
    gx, gy = lax.axis_index("gx"), lax.axis_index("gy")
    me = gx * pn.ny + gy
    peers, k, lines = pn.peers, pn.k, pn.lines

    def dev(p):
        return {"gx": lax.div(p, pn.ny), "gy": lax.rem(p, pn.ny)}

    def remote(src, dst, ssem, rsem, p):
        return pltpu.make_async_remote_copy(
            src_ref=src, dst_ref=dst, send_sem=ssem, recv_sem=rsem,
            device_id=dev(p), device_id_type=pl.DeviceIdType.MESH,
        )

    def others(body):
        def step(d, _):
            body(lax.rem(me + d, peers))
            return 0
        lax.fori_loop(1, peers, step, 0)

    barrier = pltpu.get_barrier_semaphore()
    others(lambda p: pl.semaphore_signal(
        barrier, inc=1, device_id=dev(p), device_id_type=pl.DeviceIdType.MESH))

    lane = lax.broadcasted_iota(I32, (8, LN), 1)
    sub = lax.broadcasted_iota(I32, (8, LN), 0)
    iota_row = lax.broadcasted_iota(I32, (256, LN), 0).astype(F32).astype(BF16)
    one, zero = jnp.ones((), BF16), jnp.zeros((), BF16)

    def lsum(x):
        return jnp.sum(x, axis=1, keepdims=True)

    def ssum(x):
        return jnp.sum(x, axis=0, keepdims=True)

    def fold(v):
        for h in (4, 2, 1):
            low = (sub & h) == 0
            n = len(v) // 2
            nxt = []
            for i in range(n):
                keep = jnp.where(low, v[i], v[i + n])
                give = jnp.where(low, v[i + n], v[i])
                if h == 4:
                    moved = pltpu.roll(give, 4, 0)
                else:
                    moved = jnp.where(low, pltpu.roll(give, 8 - h, 0), pltpu.roll(give, h, 0))
                nxt.append(keep + moved)
            v = nxt
        return v[0]

    def pick(parts, bits):
        for bit in bits:
            parts = [jnp.where(bit, parts[2 * j + 1], parts[2 * j]) for j in range(len(parts) // 2)]
        return parts[0]

    def onehot(row):
        return jnp.where(iota_row == row, one, zero)

    nrb[me] = nr_ref[...]

    ext = []
    for a in range(3):
        rows_b = jnp.broadcast_to(b_ref[a : a + 1, :], (8, pn.rows))
        pad = jnp.zeros((LN // 2 - k - 8, pn.rows), F32)
        ext.append(jnp.concatenate([c_ref[a * k : (a + 1) * k, :], rows_b, pad], axis=0))
    gram = None
    for a in range(3):
        hi = ext[a].astype(BF16)
        both = jnp.concatenate([hi, (ext[a] - hi.astype(F32)).astype(BF16)], axis=0)
        g = lax.dot_general(both, both, NT, preferred_element_type=F32)
        gram = g if gram is None else gram + g
    gram = gram[0 : LN // 2] + gram[LN // 2 :]
    gram = gram + pltpu.roll(gram, LN // 2, 1)
    lane16 = lax.broadcasted_iota(I32, (16, LN), 1)
    packet = jnp.zeros((16, LN), F32)
    third = k // 3
    groups = [gram[third * i : third * (i + 1)] for i in range(3)]
    tail = jnp.concatenate([gram[k : k + 8], gram[k : k + 8]], axis=0)
    starts = (0, third, 3 * third, 6 * third)
    for i in range(3):
        moved = pltpu.roll(groups[i], starts[i], 1) if starts[i] else groups[i]
        inside = jnp.logical_and(lane16 >= starts[i], lane16 < starts[i + 1])
        packet = jnp.where(inside, moved, packet)
        packet = jnp.where(lane16 == starts[3] + i, pltpu.roll(groups[i], starts[3] + i - k, 1), packet)
    packet = jnp.where(lane16 == starts[3] + 3, pltpu.roll(tail, starts[3] + 3 - k, 1), packet)
    gpk[...] = packet
    grcv[me] = packet

    pl.semaphore_wait(barrier, peers - 1)
    others(lambda p: remote(nr_ref, nrb.at[me], n_s.at[p], n_r.at[me], p).start())
    others(lambda p: remote(gpk, grcv.at[me], g_s.at[p], g_r.at[me], p).start())

    for t in range(lines):
        at = slice(t * LN, (t + 1) * LN)
        opd[pl.ds(t, pn.op_rows, stride=lines), :] = op_ref[:, at]
        bd[pl.ds(t, 3, stride=lines), :] = b_ref[:, at]
    load = [bd[a * lines : (a + 1) * lines, :] for a in range(3)]

    for cb in range(pn.blocks):
        iacc[cb] = jnp.zeros((256, 256), F32)
    lane_row = lax.broadcasted_iota(I32, (1, LN), 1)

    def invert_one(i):
        d = lax.rem(me + i, peers)

        @pl.when(i > 0)
        def _():
            remote(nr_ref, nrb.at[d], n_s.at[d], n_r.at[d], d).wait_recv()

        zs = []
        core = lax.rem(d, pn.ny)
        first = (core * LN + lane_row).astype(F32).astype(BF16)
        for s in range(lines):
            row = nrb[d, s : s + 1, :]
            zrow = lax.bitwise_and(row, LN - 1).astype(F32).astype(BF16)
            hit = iota_row[0:LN] == zrow
            line = lax.div(d, pn.ny) * lines + s - pn.qh
            second = jnp.full((1, LN), 0, I32) + line
            second = second.astype(F32).astype(BF16)
            zs.append(jnp.concatenate([jnp.where(hit, first, zero), jnp.where(hit, second, zero)], axis=0))
        z = jnp.concatenate(zs, axis=1)
        for cb in range(pn.blocks):
            cs = []
            for s in range(lines):
                crow = lax.shift_right_logical(nrb[d, s : s + 1, :], 7) - cb * 256
                crow = jnp.clip(crow, -1, 256).astype(F32).astype(BF16)
                cs.append(onehot(crow))
            c = jnp.concatenate(cs, axis=1)
            iacc[cb] += lax.dot_general(z, c, NT, preferred_element_type=F32)

    def invert(j, _):
        for i in range(4):
            invert_one(4 * j + i)
        return 0

    lax.fori_loop(0, peers // 4, invert, 0)
    for cb in range(pn.blocks):
        itab[cb] = iacc[cb].astype(BF16)

    others(lambda p: remote(gpk, grcv.at[p], g_s.at[p], g_r.at[p], p).wait_recv())
    total = grcv[0]
    for d in range(1, peers):
        total = total + grcv[d]
    ke = k + 8
    lanes_e = lax.broadcasted_iota(I32, (ke, LN), 1)
    rows_e = lax.broadcasted_iota(I32, (ke, LN), 0)
    low = []
    for i in range(3):
        block = pltpu.roll(total, LN - starts[i], 1) if starts[i] else total
        block = jnp.where(lane16 < third * (i + 1), block, 0.0)
        load_col = pltpu.roll(total, LN - (starts[3] + i) + k, 1)
        low.append(jnp.where(lane16 == k, load_col, block))
    square = pltpu.roll(total, LN - (starts[3] + 3) + k, 1)
    low.append(jnp.where(lane16 == k, square, 0.0)[0:8])
    low.append(jnp.zeros((LN - ke, LN), F32))
    low = jnp.concatenate(low, axis=0)
    high = jnp.transpose(low)
    low, high = low[0:ke], high[0:ke]
    diag = lax.div(rows_e, third) == lax.div(lanes_e, third)
    lower = jnp.logical_or(diag, lanes_e <= rows_e)
    mat = jnp.where(jnp.logical_or(lower, lanes_e == k), low, high)
    mat = jnp.where(jnp.logical_and(rows_e == k, lanes_e < k), high, mat)
    for i in range(k):
        row = mat[i : i + 1, :]
        col = jnp.broadcast_to(mat[:, i : i + 1], (ke, LN))
        at = lanes_e == i
        scaled = jnp.where(lane_row == i, 1.0, row) / col[i : i + 1]
        inner = jnp.where(at, 0.0, mat) - col * scaled
        mat = jnp.where(rows_e == i, scaled, inner)
    ginv = jnp.where(lanes_e < k, mat, 0.0)[0:k]
    z0 = jnp.broadcast_to(mat[0:k, k : k + 1], (k, LN))
    beta = jnp.sqrt(jnp.broadcast_to(mat[k : k + 1, k : k + 1], (1, LN)))

    def combine(ref, z):
        out = []
        for a in range(3):
            sums = []
            for t in range(lines):
                s = None
                for g in range(k // 8):
                    term = ref[a * k + 8 * g : a * k + 8 * g + 8, t * LN : (t + 1) * LN] * z[8 * g : 8 * g + 8]
                    s = term if s is None else s + term
                sums.append(s)
            out.append(fold(sums))
        return out

    half_n = pn.nx // 2
    side = lax.div(gx, half_n)

    def spread(phase, v):
        for a in range(3):
            vsnd[phase, a] = v[a]
            vb[phase, gy, a, pl.ds(pl.multiple_of(gx * lines, 8), 8), :] = v[a]
        mine = pl.ds(pl.multiple_of(gx * lines, 8), 8)
        half = half_n * pn.ny
        at = me - side * half

        def send(p):
            remote(vsnd.at[phase], vb.at[phase, gy, :, mine, :], v_s.at[phase, p], v_r.at[phase, me], p).start()

        def near(i, _):
            send(side * half + lax.rem(at + i, half))
            return 0

        def far(i, _):
            send((1 - side) * half + lax.rem(at + i, half))
            return 0

        lax.fori_loop(1, half, near, 0)
        lax.fori_loop(0, half, far, 0)

    def arrive(phase, half):
        def step(i, _):
            p = half * half_n * pn.ny + i
            at = pl.ds(pl.multiple_of(lax.div(p, pn.ny) * lines, 8), 8)

            @pl.when(p != me)
            def _():
                remote(vsnd.at[phase], vb.at[phase, lax.rem(p, pn.ny), :, at, :],
                       v_s.at[phase, p], v_r.at[phase, p], p).wait_recv()
            return 0
        lax.fori_loop(0, half_n * pn.ny, step, 0)
        begin = pl.ds(pl.multiple_of(half * pn.qh, 8), pn.qh)
        for b in range(3):
            xs = [vb[phase, core, b, begin, :] for core in range(pn.ny)]
            top = functools.reduce(jnp.maximum, [jnp.abs(x) for x in xs])
            top = jnp.maximum(jnp.max(top, axis=1, keepdims=True), 1e-30)
            scale = 240.0 / top
            sinv[b * pn.qh : (b + 1) * pn.qh, :] = jnp.broadcast_to(top * (1.0 / 240.0), (pn.qh, LN))
            for core in range(pn.ny):
                x = xs[core] * scale
                for piece in range(3):
                    part = x.astype(F8)
                    x = x - part.astype(F32)
                    at = (piece * 3 + b) * pn.qh
                    tab[at : at + pn.qh, core * LN : (core + 1) * LN] = part

    levels = pn.qh.bit_length() - 4
    rest = ~((pn.qh - 1) & ~7)

    def gather(kk, half):
        vals = [[None] * lines for _ in range(3)]
        for c in range(lines // 2):
            w = jnp.concatenate(
                [onehot(kidx[kk, 2 * c + t : 2 * c + t + 1, :].astype(BF16)) for t in range(2)], axis=1).astype(F8)
            r = jnp.dot(tab[...], w, preferred_element_type=F32)
            for t in range(2):
                q = jnp.broadcast_to(qidx[kk, 2 * c + t : 2 * c + t + 1, :], (8, LN)) - half * pn.qh
                bits = [lax.bitwise_and(q, 8 << i) != 0 for i in range(levels)]
                here = lax.bitwise_and(q, rest) == sub
                lanes_t = slice(t * LN, (t + 1) * LN)
                for b in range(3):
                    parts = []
                    for i in range(pn.qh // 8):
                        at = b * pn.qh + i * 8
                        ps = [r[at + 3 * pn.qh * j : at + 3 * pn.qh * j + 8, lanes_t] for j in range(3)]
                        parts.append((ps[0] + (ps[1] + ps[2])) * sinv[at : at + 8, :])
                    vals[b][2 * c + t] = jnp.where(here, pick(parts, bits), 0.0)
        return [fold(vals[b]) for b in range(3)]

    def coef(i):
        return opd[pl.ds(pl.multiple_of(i * lines, 8), 8), :]

    def apply_half(half):
        def step(i, out):
            for u in range(3):
                kk = 3 * i + u
                g = gather(kk, half)
                out = tuple(
                    out[a] + (coef(kk * 9 + a * 3) * g[0] + coef(kk * 9 + a * 3 + 1) * g[1] + coef(kk * 9 + a * 3 + 2) * g[2])
                    for a in range(3))
            return out
        return lax.fori_loop(0, pn.op_rows // 27, step, (jnp.zeros((8, LN), F32),) * 3)

    def apply_op(phase, extra=False):
        def step(i, carry):
            half = lax.rem(side + i, 2)
            arrive(phase, half)
            part = apply_half(half)
            if extra:
                part = part + tuple(gather(pn.op_rows // 9, half))
            return tuple(x + y for x, y in zip(carry, part))
        return lax.fori_loop(0, 2, step, (jnp.zeros((8, LN), F32),) * (6 if extra else 3))

    def dot3(p, q):
        return ssum(p[0] * q[0] + p[1] * q[1] + p[2] * q[2])

    def sums_of(phase, w, vectors):
        for a in range(3):
            wd[a] = w[a]
        bc = [[jnp.broadcast_to(wd[a, t : t + 1, :], (8, LN)) for t in range(lines)] for a in range(3)]
        for g in range(k // 8):
            s = None
            for a in range(3):
                for t in range(lines):
                    term = c_ref[a * k + 8 * g : a * k + 8 * g + 8, t * LN : (t + 1) * LN] * bc[a][t]
                    s = term if s is None else s + term
            mred[8 * g : 8 * g + 8, :] = s
        tail_rows = jnp.zeros((8, LN), F32)
        for i, vector in enumerate(vectors + [w]):
            tail_rows = jnp.where(sub == i, dot3(vector, w), tail_rows)
        mred[k : k + 8, :] = tail_rows
        mred[k + 8 :, :] = jnp.zeros((LN - k - 8, LN), F32)
        mine_row = lax.dot_general(jnp.ones((8, LN), F32), mred[...], NT, precision=HIGH, preferred_element_type=F32)[0:1]
        rsnd[phase] = mine_row
        rrcv[phase, me] = mine_row
        others(lambda p: remote(rsnd.at[phase], rrcv.at[phase, me], r_s.at[phase, p], r_r.at[phase, me], p).start())
        others(lambda p: remote(rsnd.at[phase], rrcv.at[phase, p], r_s.at[phase, p], r_r.at[phase, p], p).wait_recv())
        prow = jnp.sum(rrcv[phase], axis=0)
        pcol = lsum(jnp.where(lanes_e == rows_e, prow, 0.0))
        z = lsum(ginv * prow)
        pz = ssum(pcol[0:k] * z)
        pcol = jnp.broadcast_to(pcol, (ke, LN))
        return jnp.broadcast_to(z, (k, LN)), jnp.broadcast_to(pz, (1, LN)), [pcol[k + i : k + i + 1] for i in range(3)]

    part = combine(c_ref, z0)
    v1 = [(load[a] - part[a]) / beta for a in range(3)]
    spread(0, v1)

    nr = nr_ref[...]
    x_at = lax.div(nr, pn.height * LN)
    y_at = lax.bitwise_and(lax.shift_right_logical(nr, 7), pn.height - 1)
    z_at = lax.bitwise_and(nr, LN - 1)
    zl = LN.bit_length() - 4

    def look(crow_of, zrow_of, shifts):
        vals = [[[None] * lines for _ in range(2)] for _ in shifts]
        for c in range(lines // 2):
            r = None
            for cb in range(pn.blocks):
                w = jnp.concatenate(
                    [onehot(jnp.clip(crow_of(2 * c + t) - cb * 256, -1, 256).astype(F32).astype(BF16)) for t in range(2)],
                    axis=1)
                d = jnp.dot(itab[cb], w, preferred_element_type=F32)
                r = d if r is None else r + d
            for t in range(2):
                for i, dz in enumerate(shifts):
                    zq = jnp.broadcast_to(zrow_of(2 * c + t), (8, LN)) + dz
                    bits = [lax.bitwise_and(zq, 8 << j) != 0 for j in range(zl)]
                    here = lax.bitwise_and(zq, 7) == sub
                    for p in range(2):
                        parts = [r[p * LN + 8 * j : p * LN + 8 * j + 8, t * LN : (t + 1) * LN] for j in range(LN // 8)]
                        vals[i][p][2 * c + t] = jnp.where(here, pick(parts, bits), 0.0)
        return [[fold(vals[i][p]) for p in range(2)] for i in range(len(shifts))]

    def neighbours(j, _):
        dx = lax.div(j, 3) - 1
        dy = lax.rem(j, 3) - 1
        found = look(
            lambda t: lax.shift_right_logical(nr_ref[t : t + 1, :], 7) + (dx * pn.height + dy),
            lambda t: lax.bitwise_and(nr_ref[t : t + 1, :], LN - 1),
            (-1, 0, 1))
        xs, ys = x_at + dx, y_at + dy
        inside = jnp.logical_and(
            jnp.logical_and(xs >= 0, xs < pn.nx), jnp.logical_and(ys >= 0, ys < pn.height))
        for i, dz in enumerate((-1, 0, 1)):
            zs = z_at + dz
            good = jnp.logical_and(inside, jnp.logical_and(zs >= 0, zs < LN))
            kidx[j * 3 + i] = found[i][0]
            qidx[j * 3 + i] = jnp.where(good, found[i][1].astype(I32) + pn.qh, -1)
        return 0

    lax.fori_loop(0, 9, neighbours, 0)
    own = look(
        lambda t: jnp.zeros((1, LN), I32) + (me * lines + t), lambda t: lane_row, (0,))
    kidx[pn.op_rows // 9] = own[0][0]
    qidx[pn.op_rows // 9] = own[0][1].astype(I32) + pn.qh

    w1 = apply_op(0)
    z1, pz, (h11, ww, _) = sums_of(0, w1, [v1])
    h21 = jnp.sqrt(ww - pz - h11 * h11)
    part = combine(c_ref, z1)
    v2 = [(w1[a] - part[a] - h11 * v1[a]) / h21 for a in range(3)]
    spread(1, v2)
    w2 = apply_op(1)
    z2, pz, (h12, h22, ww) = sums_of(1, w2, [v1, v2])
    h32 = jnp.sqrt(ww - pz - h12 * h12 - h22 * h22)
    m11 = h11 * h11 + h21 * h21
    m12 = h11 * h12 + h21 * h22
    m22 = h12 * h12 + h22 * h22 + h32 * h32
    g_one, g_two = beta * h11, beta * h12
    determ = m11 * m22 - m12 * m12
    y_one = (m22 * g_one - m12 * g_two) / determ
    y_two = (m11 * g_two - m12 * g_one) / determ
    ut = combine(u_ref, z0 - y_one * z1 - y_two * z2)
    spread(2, [ut[a] + y_one * v1[a] + y_two * v2[a] for a in range(3)])
    out = apply_op(2, extra=True)
    spread(3, [load[a] - out[a] for a in range(3)])
    for a in range(3):
        sol_ref[a] = out[3 + a]

    def last(i, carry):
        half = lax.rem(side + i, 2)
        arrive(3, half)
        return tuple(x + y for x, y in zip(carry, gather(pn.op_rows // 9, half)))

    out = lax.fori_loop(0, 2, last, (jnp.zeros((8, LN), F32),) * 3)
    for a in range(3):
        res_ref[a] = out[a]

    others(lambda p: remote(nr_ref, nrb.at[me], n_s.at[p], n_r.at[me], p).wait_send())
    others(lambda p: remote(gpk, grcv.at[me], g_s.at[p], g_r.at[me], p).wait_send())
    mine = pl.ds(pl.multiple_of(gx * lines, 8), 8)
    for phase in range(2):
        others(lambda p: remote(rsnd.at[phase], rrcv.at[phase, me], r_s.at[phase, p], r_r.at[phase, me], p).wait_send())
    for phase in range(4):
        others(lambda p: remote(
            vsnd.at[phase], vb.at[phase, gy, :, mine, :], v_s.at[phase, p], v_r.at[phase, me], p).wait_send())


def body(nx, ny, operator, basis_u, basis_c, right_side, new_rows):
    rows = operator.shape[1]
    pn = Plan(nx, ny, rows, operator.shape[0], basis_u.shape[0])
    n, lines = pn.peers, pn.lines
    vmem, dma = pltpu.VMEM, pltpu.SemaphoreType.DMA
    out = jax.ShapeDtypeStruct((3, lines, LN), F32)
    whole = pl.BlockSpec(memory_space=pltpu.VMEM)
    points = pn.op_rows // 9 + 1
    sol, res = pl.pallas_call(
        functools.partial(kernel, pn),
        out_shape=(out, out),
        in_specs=[whole] * 5,
        out_specs=(whole, whole),
        scratch_shapes=[
            vmem((pn.op_rows * lines, LN), F32),
            vmem((3 * lines, LN), F32),
            vmem((n, lines, LN), I32),
            vmem((pn.blocks, 256, 256), F32),
            vmem((pn.blocks, 256, 256), BF16),
            vmem((points, lines, LN), F32),
            vmem((points, lines, LN), I32),
            vmem((9 * pn.qh, 256), F8),
            vmem((3 * pn.qh, LN), F32),
            vmem((3, lines, LN), F32),
            vmem((16, LN), F32),
            vmem((n, 16, LN), F32),
            vmem((LN, LN), F32),
            vmem((2, 1, LN), F32),
            vmem((2, n, 1, LN), F32),
            vmem((4, 3, lines, LN), F32),
            vmem((4, ny, 3, pn.q, LN), F32),
            dma((n,)), dma((n,)),
            dma((n,)), dma((n,)),
            dma((2, n)), dma((2, n)),
            dma((4, n)), dma((4, n)),
        ],
        compiler_params=pltpu.CompilerParams(
            collective_id=0, has_side_effects=True, vmem_limit_bytes=60 << 20
        ),
        name="solve",
    )(operator, basis_u, basis_c, right_side, new_rows.reshape(lines, LN))
    return sol.reshape(3, rows), res.reshape(3, rows)


def solution(mesh):
    split = P(None, ("gx", "gy"))
    return jax.shard_map(
        functools.partial(body, mesh.shape["gx"], mesh.shape["gy"]),
        mesh=mesh,
        in_specs=(split, split, split, split, P(("gx", "gy"))),
        out_specs=(split, split),
        check_vma=False,
    )
```

```python
import functools

import jax
import jax.numpy as jnp
from jax import lax
from jax.experimental import pallas as pl
from jax.experimental.pallas import tpu as pltpu
from jax.sharding import PartitionSpec as P

LN = 128
F32 = jnp.float32
BF16 = jnp.bfloat16
I32 = jnp.int32
F8 = jnp.float8_e4m3fn
HIGH = lax.Precision.HIGHEST
NT = (((1,), (1,)), ((), ()))


class Plan:
    def __init__(self, nx, ny, rows, op_rows, basis_rows):
        self.nx, self.ny, self.rows = nx, ny, rows
        self.peers = nx * ny
        self.k = basis_rows // 3
        self.op_rows, self.basis_rows = op_rows, basis_rows
        self.lines = rows // LN
        self.q = nx * self.lines
        self.qh = self.q // 2
        self.cols = self.peers * self.lines
        self.blocks = self.cols // 256
        self.height = ny * self.lines


def kernel(
    pn, op_hbm, u_hbm, c_hbm, b_ref, nr_ref, sol_ref, res_ref,
    op_ref, u_ref, c_ref, opd, bd, nrb, inv, invb, itab, kidx, qidx, tab, sinv, wd, gpk, grcv, mred, rsnd, rrcv, vsnd, vb,
    in_s, n_s, n_r, i_s, i_r, g_s, g_r, r_s, r_r, v_s, v_r,
):
    gx, gy = lax.axis_index("gx"), lax.axis_index("gy")
    me = gx * pn.ny + gy
    peers, k, lines = pn.peers, pn.k, pn.lines

    def dev(p):
        return {"gx": lax.div(p, pn.ny), "gy": lax.rem(p, pn.ny)}

    def remote(src, dst, ssem, rsem, p):
        return pltpu.make_async_remote_copy(
            src_ref=src, dst_ref=dst, send_sem=ssem, recv_sem=rsem,
            device_id=dev(p), device_id_type=pl.DeviceIdType.MESH,
        )

    def others(body):
        def step(d, _):
            body(lax.rem(me + d, peers))
            return 0
        lax.fori_loop(1, peers, step, 0)

    def fetch(src, dst, parts, first):
        size = src.shape[0] // 8 // parts * 8
        copies = []
        for i in range(parts):
            at = pl.ds(i * size, size if i < parts - 1 else src.shape[0] - i * size)
            copies.append(pltpu.make_async_copy(src.at[at, :], dst.at[at, :], in_s.at[first + i]))
            copies[-1].start()
        return copies

    barrier = pltpu.get_barrier_semaphore()
    others(lambda p: pl.semaphore_signal(
        barrier, inc=1, device_id=dev(p), device_id_type=pl.DeviceIdType.MESH))

    c_in = fetch(c_hbm, c_ref, 3, 0)
    op_in = fetch(op_hbm, op_ref, 3, 3)
    u_in = fetch(u_hbm, u_ref, 3, 6)
    sub = lax.broadcasted_iota(I32, (8, LN), 0)
    iota_row = lax.broadcasted_iota(I32, (256, LN), 0).astype(F32).astype(BF16)
    one, zero = jnp.ones((), BF16), jnp.zeros((), BF16)

    def lsum(x):
        return jnp.sum(x, axis=1, keepdims=True)

    def ssum(x):
        return jnp.sum(x, axis=0, keepdims=True)

    def fold(v):
        for h in (4, 2, 1):
            low = (sub & h) == 0
            n = len(v) // 2
            nxt = []
            for i in range(n):
                keep = jnp.where(low, v[i], v[i + n])
                give = jnp.where(low, v[i + n], v[i])
                if h == 4:
                    moved = pltpu.roll(give, 4, 0)
                else:
                    moved = jnp.where(low, pltpu.roll(give, 8 - h, 0), pltpu.roll(give, h, 0))
                nxt.append(keep + moved)
            v = nxt
        return v[0]

    def pick(parts, bits):
        for bit in bits:
            parts = [jnp.where(bit, parts[2 * j + 1], parts[2 * j]) for j in range(len(parts) // 2)]
        return parts[0]

    def onehot(row):
        return jnp.where(iota_row == row, one, zero)

    nrb[me] = nr_ref[...]

    for copy in c_in:
        copy.wait()
    ext = []
    for a in range(3):
        rows_b = jnp.broadcast_to(b_ref[a : a + 1, :], (8, pn.rows))
        pad = jnp.zeros((LN // 2 - k - 8, pn.rows), F32)
        ext.append(jnp.concatenate([c_ref[a * k : (a + 1) * k, :], rows_b, pad], axis=0))
    gram = None
    for a in range(3):
        hi = ext[a].astype(BF16)
        both = jnp.concatenate([hi, (ext[a] - hi.astype(F32)).astype(BF16)], axis=0)
        g = lax.dot_general(both, both, NT, preferred_element_type=F32)
        gram = g if gram is None else gram + g
    gram = gram[0 : LN // 2] + gram[LN // 2 :]
    gram = gram + pltpu.roll(gram, LN // 2, 1)
    lane16 = lax.broadcasted_iota(I32, (16, LN), 1)
    packet = jnp.zeros((16, LN), F32)
    third = k // 3
    groups = [gram[third * i : third * (i + 1)] for i in range(3)]
    tail = jnp.concatenate([gram[k : k + 8], gram[k : k + 8]], axis=0)
    starts = (0, third, 3 * third, 6 * third)
    for i in range(3):
        moved = pltpu.roll(groups[i], starts[i], 1) if starts[i] else groups[i]
        inside = jnp.logical_and(lane16 >= starts[i], lane16 < starts[i + 1])
        packet = jnp.where(inside, moved, packet)
        packet = jnp.where(lane16 == starts[3] + i, pltpu.roll(groups[i], starts[3] + i - k, 1), packet)
    packet = jnp.where(lane16 == starts[3] + 3, pltpu.roll(tail, starts[3] + 3 - k, 1), packet)
    gpk[...] = packet
    grcv[me] = packet

    pl.semaphore_wait(barrier, peers - 1)
    others(lambda p: remote(nr_ref, nrb.at[me], n_s.at[p], n_r.at[me], p).start())
    others(lambda p: remote(gpk, grcv.at[me], g_s.at[p], g_r.at[me], p).start())

    for t in range(lines):
        bd[pl.ds(t, 3, stride=lines), :] = b_ref[:, t * LN : (t + 1) * LN]
    load = [bd[a * lines : (a + 1) * lines, :] for a in range(3)]
    lane_row = lax.broadcasted_iota(I32, (1, LN), 1)

    def invert_one(i, acc):
        d = lax.rem(me + i, peers)

        @pl.when(i > 0)
        def _():
            remote(nr_ref, nrb.at[d], n_s.at[d], n_r.at[d], d).wait_recv()

        zs, cs = [], []
        first = (lax.rem(d, pn.ny) * LN + lane_row).astype(F32).astype(BF16)
        for s in range(lines):
            row = nrb[d, s : s + 1, :]
            zrow = lax.bitwise_and(row, LN - 1).astype(F32).astype(BF16)
            hit = iota_row[0:LN] == zrow
            line = jnp.zeros((1, LN), I32) + (lax.div(d, pn.ny) * lines + s - pn.qh)
            line = line.astype(F32).astype(BF16)
            zs.append(jnp.concatenate([jnp.where(hit, first, zero), jnp.where(hit, line, zero)], axis=0))
            crow = jnp.clip(lax.shift_right_logical(row, 7) - me * lines, -1, lines).astype(F32).astype(BF16)
            cs.append(jnp.where(iota_row[0:16] == crow, one, zero))
        z = jnp.concatenate(zs, axis=1)
        c = jnp.concatenate(cs, axis=1)
        return acc + lax.dot_general(z, c, NT, preferred_element_type=F32)

    def invert(j, acc):
        for i in range(4):
            acc = invert_one(4 * j + i, acc)
        return acc

    found = lax.fori_loop(0, peers // 4, invert, jnp.zeros((2 * LN, 16), F32))
    found = jnp.concatenate([found, jnp.zeros((2 * LN, LN - 16), F32)], axis=1)
    first = jnp.transpose(found[0:LN])[0:lines]
    line = jnp.transpose(found[LN:])[0:lines]
    code = first + 256.0 * (line + 1.0 * pn.qh)
    inv[...] = code
    invb[me] = code
    others(lambda p: remote(inv, invb.at[me], i_s.at[p], i_r.at[me], p).start())

    for copy in op_in + u_in:
        copy.wait()
    for t in range(lines):
        opd[pl.ds(t, pn.op_rows, stride=lines), :] = op_ref[:, t * LN : (t + 1) * LN]

    others(lambda p: remote(gpk, grcv.at[p], g_s.at[p], g_r.at[p], p).wait_recv())
    total = grcv[0]
    for d in range(1, peers):
        total = total + grcv[d]
    ke = k + 8
    lanes_e = lax.broadcasted_iota(I32, (ke, LN), 1)
    rows_e = lax.broadcasted_iota(I32, (ke, LN), 0)
    low = []
    for i in range(3):
        block = pltpu.roll(total, LN - starts[i], 1) if starts[i] else total
        block = jnp.where(lane16 < third * (i + 1), block, 0.0)
        load_col = pltpu.roll(total, LN - (starts[3] + i) + k, 1)
        low.append(jnp.where(lane16 == k, load_col, block))
    square = pltpu.roll(total, LN - (starts[3] + 3) + k, 1)
    low.append(jnp.where(lane16 == k, square, 0.0)[0:8])
    low.append(jnp.zeros((LN - ke, LN), F32))
    low = jnp.concatenate(low, axis=0)
    high = jnp.transpose(low)
    low, high = low[0:ke], high[0:ke]
    diag = lax.div(rows_e, third) == lax.div(lanes_e, third)
    lower = jnp.logical_or(diag, lanes_e <= rows_e)
    mat = jnp.where(jnp.logical_or(lower, lanes_e == k), low, high)
    mat = jnp.where(jnp.logical_and(rows_e == k, lanes_e < k), high, mat)
    for i in range(0, k, 2):
        c0 = jnp.broadcast_to(mat[:, i : i + 1], (ke, LN))
        c1 = jnp.broadcast_to(mat[:, i + 1 : i + 2], (ke, LN))
        r0 = jnp.where(lane_row == i, 1.0, jnp.where(lane_row == i + 1, 0.0, mat[i : i + 1]))
        r1 = jnp.where(lane_row == i + 1, 1.0, jnp.where(lane_row == i, 0.0, mat[i + 1 : i + 2]))
        over = 1.0 / c0[i : i + 1]
        up, down = c1[i : i + 1] * over, c0[i + 1 : i + 2] * over
        s1 = (r1 - down * r0) / (c1[i + 1 : i + 2] - c0[i + 1 : i + 2] * up)
        s0 = r0 * over - up * s1
        inner = jnp.where(lax.div(lanes_e, 2) == i // 2, 0.0, mat) - c0 * s0 - c1 * s1
        mat = jnp.where(rows_e == i, s0, jnp.where(rows_e == i + 1, s1, inner))
    ginv = jnp.where(lanes_e < k, mat, 0.0)[0:k]
    z0 = jnp.broadcast_to(mat[0:k, k : k + 1], (k, LN))
    beta = jnp.sqrt(jnp.broadcast_to(mat[k : k + 1, k : k + 1], (1, LN)))

    def combine(ref, z):
        out = []
        for a in range(3):
            sums = []
            for t in range(lines):
                s = None
                for g in range(k // 8):
                    term = ref[a * k + 8 * g : a * k + 8 * g + 8, t * LN : (t + 1) * LN] * z[8 * g : 8 * g + 8]
                    s = term if s is None else s + term
                sums.append(s)
            out.append(fold(sums))
        return out

    half_n = pn.nx // 2
    half_w = half_n * pn.ny
    side = lax.div(gx, half_n)

    def spread(phase, v):
        for a in range(3):
            vsnd[phase, a] = v[a]
            vb[phase, gy, a, pl.ds(pl.multiple_of(gx * lines, 8), 8), :] = v[a]
        mine = pl.ds(pl.multiple_of(gx * lines, 8), 8)
        def send(p):
            remote(vsnd.at[phase], vb.at[phase, gy, :, mine, :], v_s.at[phase, p], v_r.at[phase, me], p).start()

        def near(i, _):
            send(side * half_w + lax.rem(me - side * half_w + i, half_w))
            return 0

        def far(i, _):
            send(((1 - side) * half_n + lax.rem(gx - side * half_n + i, half_n)) * pn.ny + gy)
            return 0

        lax.fori_loop(0, half_n, far, 0)
        lax.fori_loop(1, half_w, near, 0)

    def block(phase, p):
        at = pl.ds(pl.multiple_of(lax.div(p, pn.ny) * lines, 8), 8)
        return vb.at[phase, lax.rem(p, pn.ny), :, at, :]

    def come(phase, p):
        remote(vsnd.at[phase], block(phase, p), v_s.at[phase, p], v_r.at[phase, p], p).wait_recv()

    def far_chip(i):
        return jnp.where(side == 0, half_n + i, half_n - 1 - i)

    def relay(phase, i):
        p = far_chip(i) * pn.ny + gy
        come(phase, p)
        other = far_chip(i) * pn.ny + 1 - gy
        remote(block(phase, p), block(phase, p), v_s.at[phase, other], v_r.at[phase, p], gx * pn.ny + 1 - gy).start()

    def arrive(phase, half):
        @pl.when(half == side)
        def _():
            def step(i, _):
                come(phase, side * half_w + lax.rem(me - side * half_w + i, half_w))
                return 0
            lax.fori_loop(1, half_w, step, 0)

        @pl.when(half != side)
        def _():
            def step(i, _):
                come(phase, far_chip(i) * pn.ny + 1 - gy)
                return 0
            lax.fori_loop(0, half_n, step, 0)

        begin = pl.ds(pl.multiple_of(half * pn.qh, 8), pn.qh)
        for b in range(3):
            xs = [vb[phase, core, b, begin, :] for core in range(pn.ny)]
            top = functools.reduce(jnp.maximum, [jnp.abs(x) for x in xs])
            top = jnp.maximum(jnp.max(top, axis=1, keepdims=True), 1e-36)
            scale = 240.0 / top
            sinv[b * pn.qh : (b + 1) * pn.qh, :] = jnp.broadcast_to(top * (1.0 / 240.0), (pn.qh, LN))
            for core in range(pn.ny):
                x = xs[core] * scale
                for piece in range(3):
                    part = x.astype(F8)
                    x = x - part.astype(F32)
                    at = (piece * 3 + b) * pn.qh
                    tab[at : at + pn.qh, core * LN : (core + 1) * LN] = part

    levels = pn.qh.bit_length() - 4
    rest = ~((pn.qh - 1) & ~7)

    def gather(kk, half):
        vals = [[None] * lines for _ in range(3)]
        for c in range(lines // 2):
            w = jnp.concatenate(
                [onehot(kidx[kk, 2 * c + t : 2 * c + t + 1, :].astype(BF16)) for t in range(2)], axis=1).astype(F8)
            r = jnp.dot(tab[...], w, preferred_element_type=F32)
            for t in range(2):
                q = jnp.broadcast_to(qidx[kk, 2 * c + t : 2 * c + t + 1, :], (8, LN)) - half * pn.qh
                bits = [lax.bitwise_and(q, 8 << i) != 0 for i in range(levels)]
                here = lax.bitwise_and(q, rest) == sub
                lanes_t = slice(t * LN, (t + 1) * LN)
                for b in range(3):
                    parts = []
                    for i in range(pn.qh // 8):
                        at = b * pn.qh + i * 8
                        ps = [r[at + 3 * pn.qh * j : at + 3 * pn.qh * j + 8, lanes_t] for j in range(3)]
                        parts.append((ps[0] + (ps[1] + ps[2])) * sinv[at : at + 8, :])
                    vals[b][2 * c + t] = jnp.where(here, pick(parts, bits), 0.0)
        return [fold(vals[b]) for b in range(3)]

    def coef(i):
        return opd[pl.ds(pl.multiple_of(i * lines, 8), 8), :]

    turns = pn.op_rows // 27
    per_turn = -(-half_n // (turns - 1))

    def apply_half(phase, half):
        def step(i, out):
            for j in range(per_turn):
                @pl.when(jnp.logical_and(half == side, i * per_turn + j < half_n))
                def _():
                    relay(phase, i * per_turn + j)
            for u in range(3):
                kk = 3 * i + u
                g = gather(kk, half)
                out = tuple(
                    out[a] + (coef(kk * 9 + a * 3) * g[0] + coef(kk * 9 + a * 3 + 1) * g[1] + coef(kk * 9 + a * 3 + 2) * g[2])
                    for a in range(3))
            return out
        return lax.fori_loop(0, turns, step, (jnp.zeros((8, LN), F32),) * 3)

    def apply_op(phase, extra=False):
        def step(i, carry):
            half = lax.rem(side + i, 2)
            arrive(phase, half)
            part = apply_half(phase, half)
            if extra:
                part = part + tuple(gather(pn.op_rows // 9, half))
            return tuple(x + y for x, y in zip(carry, part))
        return lax.fori_loop(0, 2, step, (jnp.zeros((8, LN), F32),) * (6 if extra else 3))

    def dot3(p, q):
        return ssum(p[0] * q[0] + p[1] * q[1] + p[2] * q[2])

    def sums_of(phase, w, vectors):
        for a in range(3):
            wd[a] = w[a]
        bc = [[jnp.broadcast_to(wd[a, t : t + 1, :], (8, LN)) for t in range(lines)] for a in range(3)]
        for g in range(k // 8):
            s = None
            for a in range(3):
                for t in range(lines):
                    term = c_ref[a * k + 8 * g : a * k + 8 * g + 8, t * LN : (t + 1) * LN] * bc[a][t]
                    s = term if s is None else s + term
            mred[8 * g : 8 * g + 8, :] = s
        tail_rows = jnp.zeros((8, LN), F32)
        for i, vector in enumerate(vectors + [w]):
            tail_rows = jnp.where(sub == i, dot3(vector, w), tail_rows)
        mred[k : k + 8, :] = tail_rows
        mred[k + 8 :, :] = jnp.zeros((LN - k - 8, LN), F32)
        mine_row = lax.dot_general(jnp.ones((8, LN), F32), mred[...], NT, precision=HIGH, preferred_element_type=F32)[0:1]
        rsnd[phase] = mine_row
        rrcv[phase, me] = mine_row
        others(lambda p: remote(rsnd.at[phase], rrcv.at[phase, me], r_s.at[phase, p], r_r.at[phase, me], p).start())
        others(lambda p: remote(rsnd.at[phase], rrcv.at[phase, p], r_s.at[phase, p], r_r.at[phase, p], p).wait_recv())
        prow = jnp.sum(rrcv[phase], axis=0)
        pcol = lsum(jnp.where(lanes_e == rows_e, prow, 0.0))
        z = lsum(ginv * prow)
        pz = ssum(pcol[0:k] * z)
        pcol = jnp.broadcast_to(pcol, (ke, LN))
        return jnp.broadcast_to(z, (k, LN)), jnp.broadcast_to(pz, (1, LN)), [pcol[k + i : k + i + 1] for i in range(3)]

    part = combine(c_ref, z0)
    v1 = [(load[a] - part[a]) / beta for a in range(3)]
    spread(0, v1)

    others(lambda p: remote(inv, invb.at[p], i_s.at[p], i_r.at[p], p).wait_recv())
    for cb in range(pn.blocks):
        codes = invb[cb * 256 // lines : (cb + 1) * 256 // lines].reshape(256, LN).astype(I32)
        itab[cb, 0:LN, :] = jnp.transpose(lax.bitwise_and(codes, 255).astype(F32)).astype(BF16)
        itab[cb, LN:, :] = jnp.transpose((lax.shift_right_logical(codes, 8) - pn.qh).astype(F32)).astype(BF16)
    nr = nr_ref[...]
    x_at = lax.div(nr, pn.height * LN)
    y_at = lax.bitwise_and(lax.shift_right_logical(nr, 7), pn.height - 1)
    z_at = lax.bitwise_and(nr, LN - 1)
    zl = LN.bit_length() - 4

    def look(crow_of, zrow_of, shifts):
        vals = [[[None] * lines for _ in range(2)] for _ in shifts]
        for c in range(lines // 2):
            r = None
            for cb in range(pn.blocks):
                w = jnp.concatenate(
                    [onehot(jnp.clip(crow_of(2 * c + t) - cb * 256, -1, 256).astype(F32).astype(BF16)) for t in range(2)],
                    axis=1)
                d = jnp.dot(itab[cb], w, preferred_element_type=F32)
                r = d if r is None else r + d
            for t in range(2):
                for i, dz in enumerate(shifts):
                    zq = jnp.broadcast_to(zrow_of(2 * c + t), (8, LN)) + dz
                    bits = [lax.bitwise_and(zq, 8 << j) != 0 for j in range(zl)]
                    here = lax.bitwise_and(zq, 7) == sub
                    for p in range(2):
                        parts = [r[p * LN + 8 * j : p * LN + 8 * j + 8, t * LN : (t + 1) * LN] for j in range(LN // 8)]
                        vals[i][p][2 * c + t] = jnp.where(here, pick(parts, bits), 0.0)
        return [[fold(vals[i][p]) for p in range(2)] for i in range(len(shifts))]

    def neighbours(j, _):
        dx = lax.div(j, 3) - 1
        dy = lax.rem(j, 3) - 1
        found = look(
            lambda t: lax.shift_right_logical(nr_ref[t : t + 1, :], 7) + (dx * pn.height + dy),
            lambda t: lax.bitwise_and(nr_ref[t : t + 1, :], LN - 1),
            (-1, 0, 1))
        xs, ys = x_at + dx, y_at + dy
        inside = jnp.logical_and(
            jnp.logical_and(xs >= 0, xs < pn.nx), jnp.logical_and(ys >= 0, ys < pn.height))
        for i, dz in enumerate((-1, 0, 1)):
            zs = z_at + dz
            good = jnp.logical_and(inside, jnp.logical_and(zs >= 0, zs < LN))
            kidx[j * 3 + i] = found[i][0]
            qidx[j * 3 + i] = jnp.where(good, found[i][1].astype(I32) + pn.qh, -1)
        return 0

    lax.fori_loop(0, 9, neighbours, 0)
    own = look(
        lambda t: jnp.zeros((1, LN), I32) + (me * lines + t), lambda t: lane_row, (0,))
    kidx[pn.op_rows // 9] = own[0][0]
    qidx[pn.op_rows // 9] = own[0][1].astype(I32) + pn.qh

    w1 = apply_op(0)
    z1, pz, (h11, ww, _) = sums_of(0, w1, [v1])
    h21 = jnp.sqrt(ww - pz - h11 * h11)
    part = combine(c_ref, z1)
    v2 = [(w1[a] - part[a] - h11 * v1[a]) / h21 for a in range(3)]
    spread(1, v2)
    w2 = apply_op(1)
    z2, pz, (h12, h22, ww) = sums_of(1, w2, [v1, v2])
    h32 = jnp.sqrt(ww - pz - h12 * h12 - h22 * h22)
    m11 = h11 * h11 + h21 * h21
    m12 = h11 * h12 + h21 * h22
    m22 = h12 * h12 + h22 * h22 + h32 * h32
    g_one, g_two = beta * h11, beta * h12
    determ = m11 * m22 - m12 * m12
    y_one = (m22 * g_one - m12 * g_two) / determ
    y_two = (m11 * g_two - m12 * g_one) / determ
    ut = combine(u_ref, z0 - y_one * z1 - y_two * z2)
    spread(2, [ut[a] + y_one * v1[a] + y_two * v2[a] for a in range(3)])
    out = apply_op(2, extra=True)
    spread(3, [load[a] - out[a] for a in range(3)])
    for a in range(3):
        sol_ref[a] = out[3 + a]

    def pass_on(i, _):
        relay(3, i)
        return 0

    lax.fori_loop(0, half_n, pass_on, 0)

    def last(i, carry):
        half = lax.rem(side + i, 2)
        arrive(3, half)
        return tuple(x + y for x, y in zip(carry, gather(pn.op_rows // 9, half)))

    out = lax.fori_loop(0, 2, last, (jnp.zeros((8, LN), F32),) * 3)
    for a in range(3):
        res_ref[a] = out[a]

    others(lambda p: remote(nr_ref, nrb.at[me], n_s.at[p], n_r.at[me], p).wait_send())
    others(lambda p: remote(gpk, grcv.at[me], g_s.at[p], g_r.at[me], p).wait_send())
    others(lambda p: remote(inv, invb.at[me], i_s.at[p], i_r.at[me], p).wait_send())
    mine = pl.ds(pl.multiple_of(gx * lines, 8), 8)
    for phase in range(2):
        others(lambda p: remote(rsnd.at[phase], rrcv.at[phase, me], r_s.at[phase, p], r_r.at[phase, me], p).wait_send())
    for phase in range(4):
        others(lambda p: remote(
            vsnd.at[phase], vb.at[phase, gy, :, mine, :], v_s.at[phase, p], v_r.at[phase, me], p).wait_send())


def body(nx, ny, operator, basis_u, basis_c, right_side, new_rows):
    rows = operator.shape[1]
    pn = Plan(nx, ny, rows, operator.shape[0], basis_u.shape[0])
    n, lines = pn.peers, pn.lines
    vmem, dma = pltpu.VMEM, pltpu.SemaphoreType.DMA
    out = jax.ShapeDtypeStruct((3, lines, LN), F32)
    whole = pl.BlockSpec(memory_space=pltpu.VMEM)
    points = pn.op_rows // 9 + 1
    sol, res = pl.pallas_call(
        functools.partial(kernel, pn),
        out_shape=(out, out),
        in_specs=[pl.BlockSpec(memory_space=pl.ANY)] * 3 + [whole] * 2,
        out_specs=(whole, whole),
        scratch_shapes=[
            vmem((pn.op_rows, rows), F32),
            vmem((pn.basis_rows, rows), F32),
            vmem((pn.basis_rows, rows), F32),
            vmem((pn.op_rows * lines, LN), F32),
            vmem((3 * lines, LN), F32),
            vmem((n, lines, LN), I32),
            vmem((lines, LN), F32),
            vmem((n, lines, LN), F32),
            vmem((pn.blocks, 256, 256), BF16),
            vmem((points, lines, LN), F32),
            vmem((points, lines, LN), I32),
            vmem((9 * pn.qh, 256), F8),
            vmem((3 * pn.qh, LN), F32),
            vmem((3, lines, LN), F32),
            vmem((16, LN), F32),
            vmem((n, 16, LN), F32),
            vmem((LN, LN), F32),
            vmem((2, 1, LN), F32),
            vmem((2, n, 1, LN), F32),
            vmem((4, 3, lines, LN), F32),
            vmem((4, ny, 3, pn.q, LN), F32),
            dma((9,)),
            dma((n,)), dma((n,)),
            dma((n,)), dma((n,)),
            dma((n,)), dma((n,)),
            dma((2, n)), dma((2, n)),
            dma((4, n)), dma((4, n)),
        ],
        compiler_params=pltpu.CompilerParams(
            collective_id=0, has_side_effects=True, vmem_limit_bytes=60 << 20
        ),
        name="solve",
    )(operator, basis_u, basis_c, right_side, new_rows.reshape(lines, LN))
    return sol.reshape(3, rows), res.reshape(3, rows)


def solution(mesh):
    split = P(None, ("gx", "gy"))
    return jax.shard_map(
        functools.partial(body, mesh.shape["gx"], mesh.shape["gy"]),
        mesh=mesh,
        in_specs=(split, split, split, split, P(("gx", "gy"))),
        out_specs=(split, split),
        check_vma=False,
    )
```

```python
import functools

import jax
import jax.numpy as jnp
from jax import lax
from jax.experimental import pallas as pl
from jax.experimental.pallas import tpu as pltpu
from jax.sharding import PartitionSpec as P

LN = 128
F32 = jnp.float32
BF16 = jnp.bfloat16
I32 = jnp.int32
F8 = jnp.float8_e4m3fn
HIGH = lax.Precision.HIGHEST
NT = (((1,), (1,)), ((), ()))


class Plan:
    def __init__(self, nx, ny, rows, op_rows, basis_rows):
        self.nx, self.ny, self.rows = nx, ny, rows
        self.peers = nx * ny
        self.k = basis_rows // 3
        self.op_rows, self.basis_rows = op_rows, basis_rows
        self.lines = rows // LN
        self.q = nx * self.lines
        self.qh = self.q // 2
        self.cols = self.peers * self.lines
        self.blocks = self.cols // 256
        self.height = ny * self.lines


def kernel(
    pn, op_hbm, u_hbm, c_hbm, b_ref, nr_ref, sol_ref, res_ref,
    op_ref, u_ref, c_ref, opd, bd, nrb, inv, invb, itab, kidx, qidx, tab, sinv, wd, gpk, grcv, mred, rsnd, rrcv, vsnd, vb,
in_s, n_s, n_r, i_s, i_r, g_s, g_r, r_s, r_r, near_s, far_s, pass_s, near_r, far_r, pass_r,
):
    gx, gy = lax.axis_index("gx"), lax.axis_index("gy")
    me = gx * pn.ny + gy
    peers, k, lines = pn.peers, pn.k, pn.lines

    def dev(p):
        return {"gx": lax.div(p, pn.ny), "gy": lax.rem(p, pn.ny)}

    def remote(src, dst, ssem, rsem, p):
        return pltpu.make_async_remote_copy(
            src_ref=src, dst_ref=dst, send_sem=ssem, recv_sem=rsem,
            device_id=dev(p), device_id_type=pl.DeviceIdType.MESH,
        )

    def others(body):
        def step(d, _):
            body(lax.rem(me + d, peers))
            return 0
        lax.fori_loop(1, peers, step, 0)

    def fetch(src, dst, i):
        copy = pltpu.make_async_copy(src, dst, in_s.at[i])
        copy.start()
        return copy

    def all_of(ref, ssem, rsem):
        return remote(ref, ref, ssem, rsem, lax.rem(me + 1, peers))

    most = pl.ds(0, peers - 1)

    barrier = pltpu.get_barrier_semaphore()
    others(lambda p: pl.semaphore_signal(
        barrier, inc=1, device_id=dev(p), device_id_type=pl.DeviceIdType.MESH))

    c_in = fetch(c_hbm, c_ref, 0)
    op_in = fetch(op_hbm, op_ref, 1)
    u_in = fetch(u_hbm, u_ref, 2)
    sub = lax.broadcasted_iota(I32, (8, LN), 0)
    iota_row = lax.broadcasted_iota(I32, (256, LN), 0).astype(F32).astype(BF16)
    one, zero = jnp.ones((), BF16), jnp.zeros((), BF16)

    def lsum(x):
        return jnp.sum(x, axis=1, keepdims=True)

    def ssum(x):
        return jnp.sum(x, axis=0, keepdims=True)

    def fold(v):
        for h in (4, 2, 1):
            low = (sub & h) == 0
            n = len(v) // 2
            nxt = []
            for i in range(n):
                keep = jnp.where(low, v[i], v[i + n])
                give = jnp.where(low, v[i + n], v[i])
                if h == 4:
                    moved = pltpu.roll(give, 4, 0)
                else:
                    moved = jnp.where(low, pltpu.roll(give, 8 - h, 0), pltpu.roll(give, h, 0))
                nxt.append(keep + moved)
            v = nxt
        return v[0]

    def pick(parts, bits):
        for bit in bits:
            parts = [jnp.where(bit, parts[2 * j + 1], parts[2 * j]) for j in range(len(parts) // 2)]
        return parts[0]

    def onehot(row):
        return jnp.where(iota_row == row, one, zero)

    nrb[me] = nr_ref[...]

    c_in.wait()
    ext = []
    for a in range(3):
        rows_b = jnp.broadcast_to(b_ref[a : a + 1, :], (8, pn.rows))
        pad = jnp.zeros((LN // 2 - k - 8, pn.rows), F32)
        ext.append(jnp.concatenate([c_ref[a * k : (a + 1) * k, :], rows_b, pad], axis=0))
    gram = None
    for a in range(3):
        hi = ext[a].astype(BF16)
        both = jnp.concatenate([hi, (ext[a] - hi.astype(F32)).astype(BF16)], axis=0)
        g = lax.dot_general(both, both, NT, preferred_element_type=F32)
        gram = g if gram is None else gram + g
    gram = gram[0 : LN // 2] + gram[LN // 2 :]
    gram = gram + pltpu.roll(gram, LN // 2, 1)
    lane16 = lax.broadcasted_iota(I32, (16, LN), 1)
    packet = jnp.zeros((16, LN), F32)
    third = k // 3
    groups = [gram[third * i : third * (i + 1)] for i in range(3)]
    tail = jnp.concatenate([gram[k : k + 8], gram[k : k + 8]], axis=0)
    starts = (0, third, 3 * third, 6 * third)
    for i in range(3):
        moved = pltpu.roll(groups[i], starts[i], 1) if starts[i] else groups[i]
        inside = jnp.logical_and(lane16 >= starts[i], lane16 < starts[i + 1])
        packet = jnp.where(inside, moved, packet)
        packet = jnp.where(lane16 == starts[3] + i, pltpu.roll(groups[i], starts[3] + i - k, 1), packet)
    packet = jnp.where(lane16 == starts[3] + 3, pltpu.roll(tail, starts[3] + 3 - k, 1), packet)
    gpk[...] = packet
    grcv[me] = packet

    pl.semaphore_wait(barrier, peers - 1)
    others(lambda p: remote(nr_ref, nrb.at[me], n_s, n_r, p).start())
    others(lambda p: remote(gpk, grcv.at[me], g_s, g_r, p).start())

    for t in range(lines):
        bd[pl.ds(t, 3, stride=lines), :] = b_ref[:, t * LN : (t + 1) * LN]
    load = [bd[a * lines : (a + 1) * lines, :] for a in range(3)]
    lane_row = lax.broadcasted_iota(I32, (1, LN), 1)

    def invert_one(i, acc):
        d = i
        zs, cs = [], []
        first = (lax.rem(d, pn.ny) * LN + lane_row).astype(F32).astype(BF16)
        for s in range(lines):
            row = nrb[d, s : s + 1, :]
            zrow = lax.bitwise_and(row, LN - 1).astype(F32).astype(BF16)
            hit = iota_row[0:LN] == zrow
            line = jnp.zeros((1, LN), I32) + (lax.div(d, pn.ny) * lines + s - pn.qh)
            line = line.astype(F32).astype(BF16)
            zs.append(jnp.concatenate([jnp.where(hit, first, zero), jnp.where(hit, line, zero)], axis=0))
            crow = jnp.clip(lax.shift_right_logical(row, 7) - me * lines, -1, lines).astype(F32).astype(BF16)
            cs.append(jnp.where(iota_row[0:16] == crow, one, zero))
        z = jnp.concatenate(zs, axis=1)
        c = jnp.concatenate(cs, axis=1)
        return acc + lax.dot_general(z, c, NT, preferred_element_type=F32)

    def invert(j, acc):
        for i in range(4):
            acc = invert_one(4 * j + i, acc)
        return acc

    all_of(nrb.at[most], n_s, n_r).wait_recv()
    found = lax.fori_loop(0, peers // 4, invert, jnp.zeros((2 * LN, 16), F32))
    found = jnp.concatenate([found, jnp.zeros((2 * LN, LN - 16), F32)], axis=1)
    first = jnp.transpose(found[0:LN])[0:lines]
    line = jnp.transpose(found[LN:])[0:lines]
    code = first + 256.0 * (line + 1.0 * pn.qh)
    inv[...] = code
    invb[me] = code
    others(lambda p: remote(inv, invb.at[me], i_s, i_r, p).start())

    op_in.wait()
    u_in.wait()
    for t in range(lines):
        opd[pl.ds(t, pn.op_rows, stride=lines), :] = op_ref[:, t * LN : (t + 1) * LN]

    all_of(grcv.at[most], g_s, g_r).wait_recv()
    total = grcv[0]
    for d in range(1, peers):
        total = total + grcv[d]
    ke = k + 8
    lanes_e = lax.broadcasted_iota(I32, (ke, LN), 1)
    rows_e = lax.broadcasted_iota(I32, (ke, LN), 0)
    low = []
    for i in range(3):
        block = pltpu.roll(total, LN - starts[i], 1) if starts[i] else total
        block = jnp.where(lane16 < third * (i + 1), block, 0.0)
        load_col = pltpu.roll(total, LN - (starts[3] + i) + k, 1)
        low.append(jnp.where(lane16 == k, load_col, block))
    square = pltpu.roll(total, LN - (starts[3] + 3) + k, 1)
    low.append(jnp.where(lane16 == k, square, 0.0)[0:8])
    low.append(jnp.zeros((LN - ke, LN), F32))
    low = jnp.concatenate(low, axis=0)
    high = jnp.transpose(low)
    low, high = low[0:ke], high[0:ke]
    diag = lax.div(rows_e, third) == lax.div(lanes_e, third)
    lower = jnp.logical_or(diag, lanes_e <= rows_e)
    mat = jnp.where(jnp.logical_or(lower, lanes_e == k), low, high)
    mat = jnp.where(jnp.logical_and(rows_e == k, lanes_e < k), high, mat)
    for i in range(0, k, 2):
        c0 = jnp.broadcast_to(mat[:, i : i + 1], (ke, LN))
        c1 = jnp.broadcast_to(mat[:, i + 1 : i + 2], (ke, LN))
        r0 = jnp.where(lane_row == i, 1.0, jnp.where(lane_row == i + 1, 0.0, mat[i : i + 1]))
        r1 = jnp.where(lane_row == i + 1, 1.0, jnp.where(lane_row == i, 0.0, mat[i + 1 : i + 2]))
        over = 1.0 / c0[i : i + 1]
        up, down = c1[i : i + 1] * over, c0[i + 1 : i + 2] * over
        s1 = (r1 - down * r0) / (c1[i + 1 : i + 2] - c0[i + 1 : i + 2] * up)
        s0 = r0 * over - up * s1
        inner = jnp.where(lax.div(lanes_e, 2) == i // 2, 0.0, mat) - c0 * s0 - c1 * s1
        mat = jnp.where(rows_e == i, s0, jnp.where(rows_e == i + 1, s1, inner))
    ginv = jnp.where(lanes_e < k, mat, 0.0)[0:k]
    z0 = jnp.broadcast_to(mat[0:k, k : k + 1], (k, LN))
    beta = jnp.sqrt(jnp.broadcast_to(mat[k : k + 1, k : k + 1], (1, LN)))

    def combine(ref, z):
        out = []
        for a in range(3):
            sums = []
            for t in range(lines):
                s = None
                for g in range(k // 8):
                    term = ref[a * k + 8 * g : a * k + 8 * g + 8, t * LN : (t + 1) * LN] * z[8 * g : 8 * g + 8]
                    s = term if s is None else s + term
                sums.append(s)
            out.append(fold(sums))
        return out

    half_n = pn.nx // 2
    half_w = half_n * pn.ny
    side = lax.div(gx, half_n)

    def spread(phase, v):
        for a in range(3):
            vsnd[phase, a] = v[a]
            vb[phase, gy, a, pl.ds(pl.multiple_of(gx * lines, 8), 8), :] = v[a]
        mine = pl.ds(pl.multiple_of(gx * lines, 8), 8)
        def near(i, _):
            p = (side * half_w + lax.rem(me - side * half_w + i, half_w))
            remote(vsnd.at[phase], vb.at[phase, gy, :, mine, :], near_s.at[phase], near_r.at[phase], p).start()
            return 0

        def far(i, _):
            p = ((1 - side) * half_n + lax.rem(gx - side * half_n + i, half_n)) * pn.ny + gy
            remote(vsnd.at[phase], vb.at[phase, gy, :, mine, :], far_s.at[phase],
                   far_r.at[phase, gx - side * half_n], p).start()
            return 0

        lax.fori_loop(0, half_n, far, 0)
        lax.fori_loop(1, half_w, near, 0)

    def block(phase, p):
        at = pl.ds(pl.multiple_of(lax.div(p, pn.ny) * lines, 8), 8)
        return vb.at[phase, lax.rem(p, pn.ny), :, at, :]

    def rows_of(count):
        return opd.at[pl.ds(0, count * 3 * lines), :]

    def relay(phase, i):
        at = jnp.where(side == 0, i, half_n - 1 - i)
        p = ((1 - side) * half_n + at) * pn.ny + gy
        remote(vsnd.at[phase], block(phase, p), far_s.at[phase], far_r.at[phase, at], p).wait_recv()
        remote(block(phase, p), block(phase, p), pass_s.at[phase], pass_r.at[phase], gx * pn.ny + 1 - gy).start()

    def arrive(phase, half):
        @pl.when(half == side)
        def _():
            all_of(rows_of(half_w - 1), near_s.at[phase], near_r.at[phase]).wait_recv()

        @pl.when(half != side)
        def _():
            all_of(rows_of(half_n), pass_s.at[phase], pass_r.at[phase]).wait_recv()

        begin = pl.ds(pl.multiple_of(half * pn.qh, 8), pn.qh)
        for b in range(3):
            xs = [vb[phase, core, b, begin, :] for core in range(pn.ny)]
            top = functools.reduce(jnp.maximum, [jnp.abs(x) for x in xs])
            top = jnp.maximum(jnp.max(top, axis=1, keepdims=True), 1e-36)
            scale = 240.0 / top
            sinv[b * pn.qh : (b + 1) * pn.qh, :] = jnp.broadcast_to(top * (1.0 / 240.0), (pn.qh, LN))
            for core in range(pn.ny):
                x = xs[core] * scale
                for piece in range(3):
                    part = x.astype(F8)
                    x = x - part.astype(F32)
                    at = (piece * 3 + b) * pn.qh
                    tab[at : at + pn.qh, core * LN : (core + 1) * LN] = part

    levels = pn.qh.bit_length() - 4
    rest = ~((pn.qh - 1) & ~7)

    def gather(kk, half):
        vals = [[None] * lines for _ in range(3)]
        for c in range(lines // 2):
            w = jnp.concatenate(
                [onehot(kidx[kk, 2 * c + t : 2 * c + t + 1, :].astype(BF16)) for t in range(2)], axis=1).astype(F8)
            r = jnp.dot(tab[...], w, preferred_element_type=F32)
            for t in range(2):
                q = jnp.broadcast_to(qidx[kk, 2 * c + t : 2 * c + t + 1, :], (8, LN)) - half * pn.qh
                bits = [lax.bitwise_and(q, 8 << i) != 0 for i in range(levels)]
                here = lax.bitwise_and(q, rest) == sub
                lanes_t = slice(t * LN, (t + 1) * LN)
                for b in range(3):
                    parts = []
                    for i in range(pn.qh // 8):
                        at = b * pn.qh + i * 8
                        ps = [r[at + 3 * pn.qh * j : at + 3 * pn.qh * j + 8, lanes_t] for j in range(3)]
                        parts.append((ps[0] + (ps[1] + ps[2])) * sinv[at : at + 8, :])
                    vals[b][2 * c + t] = jnp.where(here, pick(parts, bits), 0.0)
        return [fold(vals[b]) for b in range(3)]

    def coef(i):
        return opd[pl.ds(pl.multiple_of(i * lines, 8), 8), :]

    turns = pn.op_rows // 27
    per_turn = -(-half_n // (turns - 1))

    def apply_half(phase, half):
        def step(i, out):
            for j in range(per_turn):
                @pl.when(jnp.logical_and(half == side, i * per_turn + j < half_n))
                def _():
                    relay(phase, i * per_turn + j)
            for u in range(3):
                kk = 3 * i + u
                g = gather(kk, half)
                out = tuple(
                    out[a] + (coef(kk * 9 + a * 3) * g[0] + coef(kk * 9 + a * 3 + 1) * g[1] + coef(kk * 9 + a * 3 + 2) * g[2])
                    for a in range(3))
            return out
        return lax.fori_loop(0, turns, step, (jnp.zeros((8, LN), F32),) * 3)

    def apply_op(phase, extra=False):
        def step(i, carry):
            half = lax.rem(side + i, 2)
            arrive(phase, half)
            part = apply_half(phase, half)
            if extra:
                part = part + tuple(gather(pn.op_rows // 9, half))
            return tuple(x + y for x, y in zip(carry, part))
        return lax.fori_loop(0, 2, step, (jnp.zeros((8, LN), F32),) * (6 if extra else 3))

    def dot3(p, q):
        return ssum(p[0] * q[0] + p[1] * q[1] + p[2] * q[2])

    def sums_of(phase, w, vectors):
        for a in range(3):
            wd[a] = w[a]
        bc = [[jnp.broadcast_to(wd[a, t : t + 1, :], (8, LN)) for t in range(lines)] for a in range(3)]
        for g in range(k // 8):
            s = None
            for a in range(3):
                for t in range(lines):
                    term = c_ref[a * k + 8 * g : a * k + 8 * g + 8, t * LN : (t + 1) * LN] * bc[a][t]
                    s = term if s is None else s + term
            mred[8 * g : 8 * g + 8, :] = s
        tail_rows = jnp.zeros((8, LN), F32)
        for i, vector in enumerate(vectors + [w]):
            tail_rows = jnp.where(sub == i, dot3(vector, w), tail_rows)
        mred[k : k + 8, :] = tail_rows
        mred[k + 8 :, :] = jnp.zeros((LN - k - 8, LN), F32)
        mine_row = lax.dot_general(jnp.ones((8, LN), F32), mred[...], NT, precision=HIGH, preferred_element_type=F32)[0:1]
        rsnd[phase] = mine_row
        rrcv[phase, me] = mine_row
        others(lambda p: remote(rsnd.at[phase], rrcv.at[phase, me], r_s.at[phase], r_r.at[phase], p).start())
        all_of(rrcv.at[phase, most], r_s.at[phase], r_r.at[phase]).wait_recv()
        prow = jnp.sum(rrcv[phase], axis=0)
        pcol = lsum(jnp.where(lanes_e == rows_e, prow, 0.0))
        z = lsum(ginv * prow)
        pz = ssum(pcol[0:k] * z)
        pcol = jnp.broadcast_to(pcol, (ke, LN))
        return jnp.broadcast_to(z, (k, LN)), jnp.broadcast_to(pz, (1, LN)), [pcol[k + i : k + i + 1] for i in range(3)]

    part = combine(c_ref, z0)
    v1 = [(load[a] - part[a]) / beta for a in range(3)]
    spread(0, v1)

    all_of(invb.at[most], i_s, i_r).wait_recv()
    for cb in range(pn.blocks):
        codes = invb[cb * 256 // lines : (cb + 1) * 256 // lines].reshape(256, LN).astype(I32)
        itab[cb, 0:LN, :] = jnp.transpose(lax.bitwise_and(codes, 255).astype(F32)).astype(BF16)
        itab[cb, LN:, :] = jnp.transpose((lax.shift_right_logical(codes, 8) - pn.qh).astype(F32)).astype(BF16)
    nr = nr_ref[...]
    x_at = lax.div(nr, pn.height * LN)
    y_at = lax.bitwise_and(lax.shift_right_logical(nr, 7), pn.height - 1)
    z_at = lax.bitwise_and(nr, LN - 1)
    zl = LN.bit_length() - 4

    def look(crow_of, zrow_of, shifts):
        vals = [[[None] * lines for _ in range(2)] for _ in shifts]
        for c in range(lines // 2):
            r = None
            for cb in range(pn.blocks):
                w = jnp.concatenate(
                    [onehot(jnp.clip(crow_of(2 * c + t) - cb * 256, -1, 256).astype(F32).astype(BF16)) for t in range(2)],
                    axis=1)
                d = jnp.dot(itab[cb], w, preferred_element_type=F32)
                r = d if r is None else r + d
            for t in range(2):
                for i, dz in enumerate(shifts):
                    zq = jnp.broadcast_to(zrow_of(2 * c + t), (8, LN)) + dz
                    bits = [lax.bitwise_and(zq, 8 << j) != 0 for j in range(zl)]
                    here = lax.bitwise_and(zq, 7) == sub
                    for p in range(2):
                        parts = [r[p * LN + 8 * j : p * LN + 8 * j + 8, t * LN : (t + 1) * LN] for j in range(LN // 8)]
                        vals[i][p][2 * c + t] = jnp.where(here, pick(parts, bits), 0.0)
        return [[fold(vals[i][p]) for p in range(2)] for i in range(len(shifts))]

    def neighbours(j, _):
        dx = lax.div(j, 3) - 1
        dy = lax.rem(j, 3) - 1
        found = look(
            lambda t: lax.shift_right_logical(nr_ref[t : t + 1, :], 7) + (dx * pn.height + dy),
            lambda t: lax.bitwise_and(nr_ref[t : t + 1, :], LN - 1),
            (-1, 0, 1))
        xs, ys = x_at + dx, y_at + dy
        inside = jnp.logical_and(
            jnp.logical_and(xs >= 0, xs < pn.nx), jnp.logical_and(ys >= 0, ys < pn.height))
        for i, dz in enumerate((-1, 0, 1)):
            zs = z_at + dz
            good = jnp.logical_and(inside, jnp.logical_and(zs >= 0, zs < LN))
            kidx[j * 3 + i] = found[i][0]
            qidx[j * 3 + i] = jnp.where(good, found[i][1].astype(I32) + pn.qh, -1)
        return 0

    lax.fori_loop(0, 9, neighbours, 0)
    own = look(
        lambda t: jnp.zeros((1, LN), I32) + (me * lines + t), lambda t: lane_row, (0,))
    kidx[pn.op_rows // 9] = own[0][0]
    qidx[pn.op_rows // 9] = own[0][1].astype(I32) + pn.qh

    w1 = apply_op(0)
    z1, pz, (h11, ww, _) = sums_of(0, w1, [v1])
    h21 = jnp.sqrt(ww - pz - h11 * h11)
    part = combine(c_ref, z1)
    v2 = [(w1[a] - part[a] - h11 * v1[a]) / h21 for a in range(3)]
    spread(1, v2)
    w2 = apply_op(1)
    z2, pz, (h12, h22, ww) = sums_of(1, w2, [v1, v2])
    h32 = jnp.sqrt(ww - pz - h12 * h12 - h22 * h22)
    m11 = h11 * h11 + h21 * h21
    m12 = h11 * h12 + h21 * h22
    m22 = h12 * h12 + h22 * h22 + h32 * h32
    g_one, g_two = beta * h11, beta * h12
    determ = m11 * m22 - m12 * m12
    y_one = (m22 * g_one - m12 * g_two) / determ
    y_two = (m11 * g_two - m12 * g_one) / determ
    ut = combine(u_ref, z0 - y_one * z1 - y_two * z2)
    spread(2, [ut[a] + y_one * v1[a] + y_two * v2[a] for a in range(3)])
    out = apply_op(2, extra=True)
    spread(3, [load[a] - out[a] for a in range(3)])
    for a in range(3):
        sol_ref[a] = out[3 + a]

    def pass_on(i, _):
        relay(3, i)
        return 0

    lax.fori_loop(0, half_n, pass_on, 0)

    def last(i, carry):
        half = lax.rem(side + i, 2)
        arrive(3, half)
        return tuple(x + y for x, y in zip(carry, gather(pn.op_rows // 9, half)))

    out = lax.fori_loop(0, 2, last, (jnp.zeros((8, LN), F32),) * 3)
    for a in range(3):
        res_ref[a] = out[a]

    all_of(nrb.at[most], n_s, n_r).wait_send()
    all_of(grcv.at[most], g_s, g_r).wait_send()
    all_of(invb.at[most], i_s, i_r).wait_send()
    for phase in range(2):
        all_of(rrcv.at[phase, most], r_s.at[phase], r_r.at[phase]).wait_send()
    for phase in range(4):
        all_of(rows_of(half_w - 1), near_s.at[phase], near_r.at[phase]).wait_send()
        all_of(rows_of(half_n), far_s.at[phase], pass_r.at[phase]).wait_send()
        all_of(rows_of(half_n), pass_s.at[phase], pass_r.at[phase]).wait_send()


def body(nx, ny, operator, basis_u, basis_c, right_side, new_rows):
    rows = operator.shape[1]
    pn = Plan(nx, ny, rows, operator.shape[0], basis_u.shape[0])
    n, lines = pn.peers, pn.lines
    vmem, dma = pltpu.VMEM, pltpu.SemaphoreType.DMA
    out = jax.ShapeDtypeStruct((3, lines, LN), F32)
    whole = pl.BlockSpec(memory_space=pltpu.VMEM)
    points = pn.op_rows // 9 + 1
    sol, res = pl.pallas_call(
        functools.partial(kernel, pn),
        out_shape=(out, out),
        in_specs=[pl.BlockSpec(memory_space=pl.ANY)] * 3 + [whole] * 2,
        out_specs=(whole, whole),
        scratch_shapes=[
            vmem((pn.op_rows, rows), F32),
            vmem((pn.basis_rows, rows), F32),
            vmem((pn.basis_rows, rows), F32),
            vmem((pn.op_rows * lines, LN), F32),
            vmem((3 * lines, LN), F32),
            vmem((n, lines, LN), I32),
            vmem((lines, LN), F32),
            vmem((n, lines, LN), F32),
            vmem((pn.blocks, 256, 256), BF16),
            vmem((points, lines, LN), F32),
            vmem((points, lines, LN), I32),
            vmem((9 * pn.qh, 256), F8),
            vmem((3 * pn.qh, LN), F32),
            vmem((3, lines, LN), F32),
            vmem((16, LN), F32),
            vmem((n, 16, LN), F32),
            vmem((LN, LN), F32),
            vmem((2, 1, LN), F32),
            vmem((2, n, 1, LN), F32),
            vmem((4, 3, lines, LN), F32),
            vmem((4, ny, 3, pn.q, LN), F32),
            dma((3,)),
            dma, dma, dma, dma, dma, dma,
            dma((2,)), dma((2,)),
            dma((4,)), dma((4,)), dma((4,)),
            dma((4,)), dma((4, nx // 2)), dma((4,)),
        ],
        compiler_params=pltpu.CompilerParams(
            collective_id=0, has_side_effects=True, vmem_limit_bytes=60 << 20
        ),
        name="solve",
    )(operator, basis_u, basis_c, right_side, new_rows.reshape(lines, LN))
    return sol.reshape(3, rows), res.reshape(3, rows)


def solution(mesh):
    split = P(None, ("gx", "gy"))
    return jax.shard_map(
        functools.partial(body, mesh.shape["gx"], mesh.shape["gy"]),
        mesh=mesh,
        in_specs=(split, split, split, split, P(("gx", "gy"))),
        out_specs=(split, split),
        check_vma=False,
    )
```

```python
import functools

import jax
import jax.numpy as jnp
from jax import lax
from jax.experimental import pallas as pl
from jax.experimental.pallas import tpu as pltpu
from jax.sharding import PartitionSpec as P

LN = 128
F32 = jnp.float32
BF16 = jnp.bfloat16
I32 = jnp.int32
F8 = jnp.float8_e4m3fn
HIGH = lax.Precision.HIGHEST
NT = (((1,), (1,)), ((), ()))


class Plan:
    def __init__(self, nx, ny, rows, op_rows, basis_rows):
        self.nx, self.ny, self.rows = nx, ny, rows
        self.peers = nx * ny
        self.k = basis_rows // 3
        self.op_rows, self.basis_rows = op_rows, basis_rows
        self.lines = rows // LN
        self.q = nx * self.lines
        self.qh = self.q // 2
        self.cols = self.peers * self.lines
        self.blocks = self.cols // 256
        self.height = ny * self.lines


def kernel(
    pn, op_hbm, u_hbm, c_hbm, b_ref, nr_ref, sol_ref, res_ref,
    op_ref, u_ref, c_ref, opd, bd, nrb, inv, invb, itab, kidx, qidx, tab, sinv, wd, gpk, grcv, mred, rsnd, rrcv, vsnd, vb,
in_s, n_s, n_r, i_s, i_r, g_s, g_r, r_s, r_r, near_s, far_s, pass_s, near_r, far_r, pass_r,
):
    gx, gy = lax.axis_index("gx"), lax.axis_index("gy")
    me = gx * pn.ny + gy
    peers, k, lines = pn.peers, pn.k, pn.lines

    def dev(p):
        return {"gx": lax.div(p, pn.ny), "gy": lax.rem(p, pn.ny)}

    def remote(src, dst, ssem, rsem, p):
        return pltpu.make_async_remote_copy(
            src_ref=src, dst_ref=dst, send_sem=ssem, recv_sem=rsem,
            device_id=dev(p), device_id_type=pl.DeviceIdType.MESH,
        )

    def others(body):
        def step(d, _):
            body(lax.rem(me + d, peers))
            return 0
        lax.fori_loop(1, peers, step, 0)

    def fetch(src, dst, i):
        copy = pltpu.make_async_copy(src, dst, in_s.at[i])
        copy.start()
        return copy

    def all_of(ref, ssem, rsem):
        return remote(ref, ref, ssem, rsem, lax.rem(me + 1, peers))

    most = pl.ds(0, peers - 1)

    barrier = pltpu.get_barrier_semaphore()
    others(lambda p: pl.semaphore_signal(
        barrier, inc=1, device_id=dev(p), device_id_type=pl.DeviceIdType.MESH))

    c_in = fetch(c_hbm, c_ref, 0)
    op_in = fetch(op_hbm, op_ref, 1)
    u_in = fetch(u_hbm, u_ref, 2)
    sub = lax.broadcasted_iota(I32, (8, LN), 0)
    iota_row = lax.broadcasted_iota(I32, (256, LN), 0).astype(F32).astype(BF16)
    one, zero = jnp.ones((), BF16), jnp.zeros((), BF16)

    def lsum(x):
        return jnp.sum(x, axis=1, keepdims=True)

    def ssum(x):
        return jnp.sum(x, axis=0, keepdims=True)

    def fold(v):
        for h in (4, 2, 1):
            low = (sub & h) == 0
            n = len(v) // 2
            nxt = []
            for i in range(n):
                keep = jnp.where(low, v[i], v[i + n])
                give = jnp.where(low, v[i + n], v[i])
                if h == 4:
                    moved = pltpu.roll(give, 4, 0)
                else:
                    moved = jnp.where(low, pltpu.roll(give, 8 - h, 0), pltpu.roll(give, h, 0))
                nxt.append(keep + moved)
            v = nxt
        return v[0]

    def pick(parts, bits):
        for bit in bits:
            parts = [jnp.where(bit, parts[2 * j + 1], parts[2 * j]) for j in range(len(parts) // 2)]
        return parts[0]

    def onehot(row):
        return jnp.where(iota_row == row, one, zero)

    nrb[me] = nr_ref[...]

    c_in.wait()
    ext = []
    for a in range(3):
        rows_b = jnp.broadcast_to(b_ref[a : a + 1, :], (8, pn.rows))
        pad = jnp.zeros((LN // 2 - k - 8, pn.rows), F32)
        ext.append(jnp.concatenate([c_ref[a * k : (a + 1) * k, :], rows_b, pad], axis=0))
    gram = None
    for a in range(3):
        hi = ext[a].astype(BF16)
        both = jnp.concatenate([hi, (ext[a] - hi.astype(F32)).astype(BF16)], axis=0)
        g = lax.dot_general(both, both, NT, preferred_element_type=F32)
        gram = g if gram is None else gram + g
    gram = gram[0 : LN // 2] + gram[LN // 2 :]
    gram = gram + pltpu.roll(gram, LN // 2, 1)
    lane16 = lax.broadcasted_iota(I32, (16, LN), 1)
    packet = jnp.zeros((16, LN), F32)
    third = k // 3
    groups = [gram[third * i : third * (i + 1)] for i in range(3)]
    tail = jnp.concatenate([gram[k : k + 8], gram[k : k + 8]], axis=0)
    starts = (0, third, 3 * third, 6 * third)
    for i in range(3):
        moved = pltpu.roll(groups[i], starts[i], 1) if starts[i] else groups[i]
        inside = jnp.logical_and(lane16 >= starts[i], lane16 < starts[i + 1])
        packet = jnp.where(inside, moved, packet)
        packet = jnp.where(lane16 == starts[3] + i, pltpu.roll(groups[i], starts[3] + i - k, 1), packet)
    packet = jnp.where(lane16 == starts[3] + 3, pltpu.roll(tail, starts[3] + 3 - k, 1), packet)
    gpk[...] = packet
    grcv[me] = packet

    pl.semaphore_wait(barrier, peers - 1)
    others(lambda p: remote(nr_ref, nrb.at[me], n_s, n_r, p).start())
    others(lambda p: remote(gpk, grcv.at[me], g_s, g_r, p).start())

    for t in range(lines):
        bd[pl.ds(t, 3, stride=lines), :] = b_ref[:, t * LN : (t + 1) * LN]
    load = [bd[a * lines : (a + 1) * lines, :] for a in range(3)]
    lane_row = lax.broadcasted_iota(I32, (1, LN), 1)

    def invert_one(i, acc):
        d = i
        zs, cs = [], []
        first = (lax.rem(d, pn.ny) * LN + lane_row).astype(F32).astype(BF16)
        for s in range(lines):
            row = nrb[d, s : s + 1, :]
            zrow = lax.bitwise_and(row, LN - 1).astype(F32).astype(BF16)
            hit = iota_row[0:LN] == zrow
            line = jnp.zeros((1, LN), I32) + (lax.div(d, pn.ny) * lines + s - pn.qh)
            line = line.astype(F32).astype(BF16)
            zs.append(jnp.concatenate([jnp.where(hit, first, zero), jnp.where(hit, line, zero)], axis=0))
            crow = jnp.clip(lax.shift_right_logical(row, 7) - me * lines, -1, lines).astype(F32).astype(BF16)
            cs.append(jnp.where(iota_row[0:16] == crow, one, zero))
        z = jnp.concatenate(zs, axis=1)
        c = jnp.concatenate(cs, axis=1)
        return acc + lax.dot_general(z, c, NT, preferred_element_type=F32)

    def invert(j, acc):
        for i in range(4):
            acc = invert_one(4 * j + i, acc)
        return acc

    op_in.wait()
    u_in.wait()
    for t in range(lines):
        opd[pl.ds(t, pn.op_rows, stride=lines), :] = op_ref[:, t * LN : (t + 1) * LN]
    all_of(nrb.at[most], n_s, n_r).wait_recv()
    found = lax.fori_loop(0, peers // 4, invert, jnp.zeros((2 * LN, 16), F32))
    found = jnp.concatenate([found, jnp.zeros((2 * LN, LN - 16), F32)], axis=1)
    first = jnp.transpose(found[0:LN])[0:lines]
    line = jnp.transpose(found[LN:])[0:lines]
    code = first + 256.0 * (line + 1.0 * pn.qh)
    inv[...] = code
    invb[me] = code
    others(lambda p: remote(inv, invb.at[me], i_s, i_r, p).start())


    all_of(grcv.at[most], g_s, g_r).wait_recv()
    total = grcv[0]
    for d in range(1, peers):
        total = total + grcv[d]
    ke = k + 8
    lanes_e = lax.broadcasted_iota(I32, (ke, LN), 1)
    rows_e = lax.broadcasted_iota(I32, (ke, LN), 0)
    low = []
    for i in range(3):
        block = pltpu.roll(total, LN - starts[i], 1) if starts[i] else total
        block = jnp.where(lane16 < third * (i + 1), block, 0.0)
        load_col = pltpu.roll(total, LN - (starts[3] + i) + k, 1)
        low.append(jnp.where(lane16 == k, load_col, block))
    square = pltpu.roll(total, LN - (starts[3] + 3) + k, 1)
    low.append(jnp.where(lane16 == k, square, 0.0)[0:8])
    low.append(jnp.zeros((LN - ke, LN), F32))
    low = jnp.concatenate(low, axis=0)
    high = jnp.transpose(low)
    low, high = low[0:ke], high[0:ke]
    diag = lax.div(rows_e, third) == lax.div(lanes_e, third)
    lower = jnp.logical_or(diag, lanes_e <= rows_e)
    mat = jnp.where(jnp.logical_or(lower, lanes_e == k), low, high)
    mat = jnp.where(jnp.logical_and(rows_e == k, lanes_e < k), high, mat)
    for i in range(0, k, 2):
        c0 = jnp.broadcast_to(mat[:, i : i + 1], (ke, LN))
        c1 = jnp.broadcast_to(mat[:, i + 1 : i + 2], (ke, LN))
        r0 = jnp.where(lane_row == i, 1.0, jnp.where(lane_row == i + 1, 0.0, mat[i : i + 1]))
        r1 = jnp.where(lane_row == i + 1, 1.0, jnp.where(lane_row == i, 0.0, mat[i + 1 : i + 2]))
        over = 1.0 / c0[i : i + 1]
        up, down = c1[i : i + 1] * over, c0[i + 1 : i + 2] * over
        s1 = (r1 - down * r0) / (c1[i + 1 : i + 2] - c0[i + 1 : i + 2] * up)
        s0 = r0 * over - up * s1
        inner = jnp.where(lax.div(lanes_e, 2) == i // 2, 0.0, mat) - c0 * s0 - c1 * s1
        mat = jnp.where(rows_e == i, s0, jnp.where(rows_e == i + 1, s1, inner))
    ginv = jnp.where(lanes_e < k, mat, 0.0)[0:k]
    z0 = jnp.broadcast_to(mat[0:k, k : k + 1], (k, LN))
    beta = jnp.sqrt(jnp.broadcast_to(mat[k : k + 1, k : k + 1], (1, LN)))

    def combine(ref, z):
        out = []
        for a in range(3):
            sums = []
            for t in range(lines):
                s = None
                for g in range(k // 8):
                    term = ref[a * k + 8 * g : a * k + 8 * g + 8, t * LN : (t + 1) * LN] * z[8 * g : 8 * g + 8]
                    s = term if s is None else s + term
                sums.append(s)
            out.append(fold(sums))
        return out

    half_n = pn.nx // 2
    half_w = half_n * pn.ny
    side = lax.div(gx, half_n)

    def spread(phase, v):
        for a in range(3):
            vsnd[phase, a] = v[a]
            vb[phase, gy, a, pl.ds(pl.multiple_of(gx * lines, 8), 8), :] = v[a]
        mine = pl.ds(pl.multiple_of(gx * lines, 8), 8)
        def near(i, _):
            p = (side * half_w + lax.rem(me - side * half_w + i, half_w))
            remote(vsnd.at[phase], vb.at[phase, gy, :, mine, :], near_s.at[phase], near_r.at[phase], p).start()
            return 0

        def far(i, _):
            p = ((1 - side) * half_n + lax.rem(gx - side * half_n + i, half_n)) * pn.ny + gy
            remote(vsnd.at[phase], vb.at[phase, gy, :, mine, :], far_s.at[phase],
                   far_r.at[phase, gx - side * half_n], p).start()
            return 0

        if phase == 3:
            lax.fori_loop(0, half_n, far, 0)
        lax.fori_loop(1, half_w, near, 0)
        if phase < 3:
            lax.fori_loop(0, half_n, far, 0)

    def block(phase, p):
        at = pl.ds(pl.multiple_of(lax.div(p, pn.ny) * lines, 8), 8)
        return vb.at[phase, lax.rem(p, pn.ny), :, at, :]

    def rows_of(count):
        return opd.at[pl.ds(0, count * 3 * lines), :]

    def relay(phase, i):
        at = jnp.where(side == 0, i, half_n - 1 - i)
        p = ((1 - side) * half_n + at) * pn.ny + gy
        remote(vsnd.at[phase], block(phase, p), far_s.at[phase], far_r.at[phase, at], p).wait_recv()
        remote(block(phase, p), block(phase, p), pass_s.at[phase], pass_r.at[phase], gx * pn.ny + 1 - gy).start()

    def arrive(phase, half):
        @pl.when(half == side)
        def _():
            all_of(rows_of(half_w - 1), near_s.at[phase], near_r.at[phase]).wait_recv()

        @pl.when(half != side)
        def _():
            all_of(rows_of(half_n), pass_s.at[phase], pass_r.at[phase]).wait_recv()

        begin = pl.ds(pl.multiple_of(half * pn.qh, 8), pn.qh)
        for b in range(3):
            xs = [vb[phase, core, b, begin, :] for core in range(pn.ny)]
            top = functools.reduce(jnp.maximum, [jnp.abs(x) for x in xs])
            top = jnp.maximum(jnp.max(top, axis=1, keepdims=True), 1e-36)
            scale = 240.0 / top
            sinv[b * pn.qh : (b + 1) * pn.qh, :] = jnp.broadcast_to(top * (1.0 / 240.0), (pn.qh, LN))
            for core in range(pn.ny):
                x = xs[core] * scale
                for piece in range(3):
                    part = x.astype(F8)
                    x = x - part.astype(F32)
                    at = (piece * 3 + b) * pn.qh
                    tab[at : at + pn.qh, core * LN : (core + 1) * LN] = part

    levels = pn.qh.bit_length() - 4
    rest = ~((pn.qh - 1) & ~7)

    def gather(kk, half):
        vals = [[None] * lines for _ in range(3)]
        for c in range(lines // 2):
            w = jnp.concatenate(
                [onehot(kidx[kk, 2 * c + t : 2 * c + t + 1, :].astype(BF16)) for t in range(2)], axis=1).astype(F8)
            r = jnp.dot(tab[...], w, preferred_element_type=F32)
            for t in range(2):
                q = jnp.broadcast_to(qidx[kk, 2 * c + t : 2 * c + t + 1, :], (8, LN)) - half * pn.qh
                bits = [lax.bitwise_and(q, 8 << i) != 0 for i in range(levels)]
                here = lax.bitwise_and(q, rest) == sub
                lanes_t = slice(t * LN, (t + 1) * LN)
                for b in range(3):
                    parts = []
                    for i in range(pn.qh // 8):
                        at = b * pn.qh + i * 8
                        ps = [r[at + 3 * pn.qh * j : at + 3 * pn.qh * j + 8, lanes_t] for j in range(3)]
                        parts.append((ps[0] + (ps[1] + ps[2])) * sinv[at : at + 8, :])
                    vals[b][2 * c + t] = jnp.where(here, pick(parts, bits), 0.0)
        return [fold(vals[b]) for b in range(3)]

    def coef(i):
        return opd[pl.ds(pl.multiple_of(i * lines, 8), 8), :]

    turns = pn.op_rows // 27
    per_turn = -(-half_n // (turns - 1))

    def apply_half(phase, half):
        def step(i, out):
            for j in range(per_turn):
                @pl.when(jnp.logical_and(half == side, i * per_turn + j < half_n))
                def _():
                    relay(phase, i * per_turn + j)
            for u in range(3):
                kk = 3 * i + u
                g = gather(kk, half)
                out = tuple(
                    out[a] + (coef(kk * 9 + a * 3) * g[0] + coef(kk * 9 + a * 3 + 1) * g[1] + coef(kk * 9 + a * 3 + 2) * g[2])
                    for a in range(3))
            return out
        return lax.fori_loop(0, turns, step, (jnp.zeros((8, LN), F32),) * 3)

    def apply_op(phase, extra=False):
        def step(i, carry):
            half = lax.rem(side + i, 2)
            arrive(phase, half)
            part = apply_half(phase, half)
            if extra:
                part = part + tuple(gather(pn.op_rows // 9, half))
            return tuple(x + y for x, y in zip(carry, part))
        return lax.fori_loop(0, 2, step, (jnp.zeros((8, LN), F32),) * (6 if extra else 3))

    def dot3(p, q):
        return ssum(p[0] * q[0] + p[1] * q[1] + p[2] * q[2])

    def sums_of(phase, w, vectors):
        for a in range(3):
            wd[a] = w[a]
        bc = [[jnp.broadcast_to(wd[a, t : t + 1, :], (8, LN)) for t in range(lines)] for a in range(3)]
        for g in range(k // 8):
            s = None
            for a in range(3):
                for t in range(lines):
                    term = c_ref[a * k + 8 * g : a * k + 8 * g + 8, t * LN : (t + 1) * LN] * bc[a][t]
                    s = term if s is None else s + term
            mred[8 * g : 8 * g + 8, :] = s
        tail_rows = jnp.zeros((8, LN), F32)
        for i, vector in enumerate(vectors + [w]):
            tail_rows = jnp.where(sub == i, dot3(vector, w), tail_rows)
        mred[k : k + 8, :] = tail_rows
        mred[k + 8 :, :] = jnp.zeros((LN - k - 8, LN), F32)
        mine_row = lax.dot_general(jnp.ones((8, LN), F32), mred[...], NT, precision=HIGH, preferred_element_type=F32)[0:1]
        rsnd[phase] = mine_row
        rrcv[phase, me] = mine_row
        others(lambda p: remote(rsnd.at[phase], rrcv.at[phase, me], r_s.at[phase], r_r.at[phase], p).start())
        all_of(rrcv.at[phase, most], r_s.at[phase], r_r.at[phase]).wait_recv()
        prow = jnp.sum(rrcv[phase], axis=0)
        pcol = lsum(jnp.where(lanes_e == rows_e, prow, 0.0))
        z = lsum(ginv * prow)
        pz = ssum(pcol[0:k] * z)
        pcol = jnp.broadcast_to(pcol, (ke, LN))
        return jnp.broadcast_to(z, (k, LN)), jnp.broadcast_to(pz, (1, LN)), [pcol[k + i : k + i + 1] for i in range(3)]

    part = combine(c_ref, z0)
    v1 = [(load[a] - part[a]) / beta for a in range(3)]
    spread(0, v1)

    all_of(invb.at[most], i_s, i_r).wait_recv()
    for cb in range(pn.blocks):
        codes = invb[cb * 256 // lines : (cb + 1) * 256 // lines].reshape(256, LN).astype(I32)
        itab[cb, 0:LN, :] = jnp.transpose(lax.bitwise_and(codes, 255).astype(F32)).astype(BF16)
        line = (lax.shift_right_logical(codes, 8) - pn.qh) * 256
        itab[cb, LN:, :] = jnp.transpose(line.astype(F32)).astype(BF16)
    nr = nr_ref[...]
    x_at = lax.div(nr, pn.height * LN)
    y_at = lax.bitwise_and(lax.shift_right_logical(nr, 7), pn.height - 1)
    z_at = lax.bitwise_and(nr, LN - 1)
    zl = LN.bit_length() - 4

    def look(crow_of, zrow_of, shifts):
        vals = [[None] * lines for _ in shifts]
        for c in range(lines // 2):
            r = None
            for cb in range(pn.blocks):
                w = jnp.concatenate(
                    [onehot(jnp.clip(crow_of(2 * c + t) - cb * 256, -1, 256).astype(F32).astype(BF16)) for t in range(2)],
                    axis=1)
                for p in range(2):
                    d = jnp.dot(itab[cb, p * LN : (p + 1) * LN, :], w, preferred_element_type=F32)
                    r = d if r is None else r + d
            for t in range(2):
                for i, dz in enumerate(shifts):
                    zq = jnp.broadcast_to(zrow_of(2 * c + t), (8, LN)) + dz
                    bits = [lax.bitwise_and(zq, 8 << j) != 0 for j in range(zl)]
                    here = lax.bitwise_and(zq, 7) == sub
                    parts = [r[8 * j : 8 * j + 8, t * LN : (t + 1) * LN] for j in range(LN // 8)]
                    vals[i][2 * c + t] = jnp.where(here, pick(parts, bits), 0.0)
        codes = [fold(vals[i]).astype(I32) + 256 * pn.qh for i in range(len(shifts))]
        return [(lax.bitwise_and(v, 255).astype(F32), lax.shift_right_arithmetic(v, 8)) for v in codes]

    def neighbours(j, _):
        dx = lax.div(j, 3) - 1
        dy = lax.rem(j, 3) - 1
        found = look(
            lambda t: lax.shift_right_logical(nr_ref[t : t + 1, :], 7) + (dx * pn.height + dy),
            lambda t: lax.bitwise_and(nr_ref[t : t + 1, :], LN - 1),
            (-1, 0, 1))
        xs, ys = x_at + dx, y_at + dy
        inside = jnp.logical_and(
            jnp.logical_and(xs >= 0, xs < pn.nx), jnp.logical_and(ys >= 0, ys < pn.height))
        for i, dz in enumerate((-1, 0, 1)):
            zs = z_at + dz
            good = jnp.logical_and(inside, jnp.logical_and(zs >= 0, zs < LN))
            kidx[j * 3 + i] = found[i][0]
            qidx[j * 3 + i] = jnp.where(good, found[i][1], -1)
        return 0

    lax.fori_loop(0, 9, neighbours, 0)
    own = look(
        lambda t: jnp.zeros((1, LN), I32) + (me * lines + t), lambda t: lane_row, (0,))
    kidx[pn.op_rows // 9] = own[0][0]
    qidx[pn.op_rows // 9] = own[0][1]

    w1 = apply_op(0)
    z1, pz, (h11, ww, _) = sums_of(0, w1, [v1])
    h21 = jnp.sqrt(ww - pz - h11 * h11)
    part = combine(c_ref, z1)
    v2 = [(w1[a] - part[a] - h11 * v1[a]) / h21 for a in range(3)]
    spread(1, v2)
    w2 = apply_op(1)
    z2, pz, (h12, h22, ww) = sums_of(1, w2, [v1, v2])
    h32 = jnp.sqrt(ww - pz - h12 * h12 - h22 * h22)
    m11 = h11 * h11 + h21 * h21
    m12 = h11 * h12 + h21 * h22
    m22 = h12 * h12 + h22 * h22 + h32 * h32
    g_one, g_two = beta * h11, beta * h12
    determ = m11 * m22 - m12 * m12
    y_one = (m22 * g_one - m12 * g_two) / determ
    y_two = (m11 * g_two - m12 * g_one) / determ
    ut = combine(u_ref, z0 - y_one * z1 - y_two * z2)
    spread(2, [ut[a] + y_one * v1[a] + y_two * v2[a] for a in range(3)])
    out = apply_op(2, extra=True)
    spread(3, [load[a] - out[a] for a in range(3)])
    for a in range(3):
        sol_ref[a] = out[3 + a]

    def pass_on(i, _):
        relay(3, i)
        return 0

    lax.fori_loop(0, half_n, pass_on, 0)

    def last(i, carry):
        half = lax.rem(side + i, 2)
        arrive(3, half)
        return tuple(x + y for x, y in zip(carry, gather(pn.op_rows // 9, half)))

    out = lax.fori_loop(0, 2, last, (jnp.zeros((8, LN), F32),) * 3)
    for a in range(3):
        res_ref[a] = out[a]

    all_of(nrb.at[most], n_s, n_r).wait_send()
    all_of(grcv.at[most], g_s, g_r).wait_send()
    all_of(invb.at[most], i_s, i_r).wait_send()
    for phase in range(2):
        all_of(rrcv.at[phase, most], r_s.at[phase], r_r.at[phase]).wait_send()
    for phase in range(4):
        all_of(rows_of(half_w - 1), near_s.at[phase], near_r.at[phase]).wait_send()
        all_of(rows_of(half_n), far_s.at[phase], pass_r.at[phase]).wait_send()
        all_of(rows_of(half_n), pass_s.at[phase], pass_r.at[phase]).wait_send()


def body(nx, ny, operator, basis_u, basis_c, right_side, new_rows):
    rows = operator.shape[1]
    pn = Plan(nx, ny, rows, operator.shape[0], basis_u.shape[0])
    n, lines = pn.peers, pn.lines
    vmem, dma = pltpu.VMEM, pltpu.SemaphoreType.DMA
    out = jax.ShapeDtypeStruct((3, lines, LN), F32)
    whole = pl.BlockSpec(memory_space=pltpu.VMEM)
    points = pn.op_rows // 9 + 1
    sol, res = pl.pallas_call(
        functools.partial(kernel, pn),
        out_shape=(out, out),
        in_specs=[pl.BlockSpec(memory_space=pl.ANY)] * 3 + [whole] * 2,
        out_specs=(whole, whole),
        scratch_shapes=[
            vmem((pn.op_rows, rows), F32),
            vmem((pn.basis_rows, rows), F32),
            vmem((pn.basis_rows, rows), F32),
            vmem((pn.op_rows * lines, LN), F32),
            vmem((3 * lines, LN), F32),
            vmem((n, lines, LN), I32),
            vmem((lines, LN), F32),
            vmem((n, lines, LN), F32),
            vmem((pn.blocks, 256, 256), BF16),
            vmem((points, lines, LN), F32),
            vmem((points, lines, LN), I32),
            vmem((9 * pn.qh, 256), F8),
            vmem((3 * pn.qh, LN), F32),
            vmem((3, lines, LN), F32),
            vmem((16, LN), F32),
            vmem((n, 16, LN), F32),
            vmem((LN, LN), F32),
            vmem((2, 1, LN), F32),
            vmem((2, n, 1, LN), F32),
            vmem((4, 3, lines, LN), F32),
            vmem((4, ny, 3, pn.q, LN), F32),
            dma((3,)),
            dma, dma, dma, dma, dma, dma,
            dma((2,)), dma((2,)),
            dma((4,)), dma((4,)), dma((4,)),
            dma((4,)), dma((4, nx // 2)), dma((4,)),
        ],
        compiler_params=pltpu.CompilerParams(
            collective_id=0, has_side_effects=True, vmem_limit_bytes=60 << 20
        ),
        name="solve",
    )(operator, basis_u, basis_c, right_side, new_rows.reshape(lines, LN))
    return sol.reshape(3, rows), res.reshape(3, rows)


def solution(mesh):
    split = P(None, ("gx", "gy"))
    return jax.shard_map(
        functools.partial(body, mesh.shape["gx"], mesh.shape["gy"]),
        mesh=mesh,
        in_specs=(split, split, split, split, P(("gx", "gy"))),
        out_specs=(split, split),
        check_vma=False,
    )
```
